32 devices in a mesh: section: 4 (over x, core), paths: 8 (over z, y).
Axes of the slice: x: 2, y: 2, z: 4, core: 2. Of those that a mesh axis runs over, the one named last changes fastest.
Arguments:
- normal_draws: float32 [8, 60, 8192], P('section', None, 'paths'), may hold values from -6 to 6
- cholesky: float32 [8, 8, 60, 60], P('section', 'paths'), as said below
- log_spot: float32 [60], replicated, may hold values from -0.2 to 0.2
- owner: int32 [8], replicated, may hold values from 0 to 7
- trade_factor: int32 [4096], replicated, may hold values from 0 to 59
- trade_set: int32 [4096], replicated, may hold values from 0 to 511
- notional: float32 [4096], replicated, may hold values from -5 to 5
- strike: float32 [4096], replicated, may hold values from 0.8 to 1.25
Outputs:
- exposure: float32 [8, 512], P('section')
The draws below stay inside these ranges and needn't reach their ends.
Inputs may be any that keep to these rules, and one draw needn't show every extreme that they name: `cholesky`: each block is lower triangular with a positive diagonal.
All inputs are finite; a program needn't handle non-finite values.
Results may differ from the reference program's by a relative error of at most 0.0001.
Values sent between devices are 32-bit elements; how exact they have to be, the bound alone decides.
No kernel may reach another device: no remote copies, remote signals or barrier semaphores. Data moves between devices by JAX's collectives and lax.ppermute only.
A program may use at most 64 MiB of HBM per device.

```python
import jax
import jax.numpy as jnp
from jax import lax

F = 60
TRADES = 4096
SETS = 512
DATES = 8
OWNERS = 8
PATHS = 8192


def draw_cholesky(key, part):
    first, second = jax.random.split(jax.random.fold_in(key, 17))
    diagonal = jax.random.uniform(first, (DATES, OWNERS, F), jnp.float32, 0.5, 1.5)
    spread = jax.random.normal(second, (DATES, OWNERS, F, F), jnp.float32) * (0.5 / F ** 0.5)
    lower = jnp.tril(spread, -1) + diagonal[..., None] * jnp.eye(F, dtype=jnp.float32)
    return (0.1 * lower).astype(jnp.float32)


def with_ends(result, own_key, low, largest):
    extent = result.shape
    place = [jax.random.randint(jax.random.fold_in(own_key, axis), (), 0, extent[axis]) for axis in range(len(extent))]
    result = result.at[tuple(place)].set(low)
    longest = extent.index(max(extent))
    place[longest] = (place[longest] + 1) % extent[longest]
    return result.at[tuple(place)].set(largest)


def level_of(key, shape, cuts, smallest, high):
    gain, own = 1.0, jax.random.fold_in(key, 6)
    for dim, parts in cuts:
        heights = jnp.exp(jax.random.uniform(jax.random.fold_in(own, dim), (parts,), jnp.float32, smallest / len(cuts), high / len(cuts)))
        gain = gain * jnp.repeat(heights, shape[dim] // parts).reshape([-1 if axis == dim else 1 for axis in range(len(shape))])
    return gain


def bell_draw(own_key, extent, deviation, most, pieces=(), held_as=jnp.bfloat16):
    factor_of = level_of(own_key, extent, pieces, -0.22, 0.18) if pieces else 1.0
    drawn = jax.random.normal(own_key, extent, jnp.float32) * deviation * factor_of
    return jnp.minimum(jnp.maximum(drawn, -most), most).astype(held_as)


def setup_inputs(seed: int = 0) -> dict:
    key_list = jax.random.split(jax.random.key(seed), 9)
    return {
        "normal_draws": bell_draw(key_list[0], (DATES, F, PATHS), 1.0, 6.0, ((0, 4), (2, 8)), jnp.float32),
        "cholesky": draw_cholesky(jax.random.fold_in(key_list[8], 71), 0),
        "log_spot": jnp.clip(jax.random.uniform(key_list[2], (F,), jnp.float32, -0.2, 0.2), -0.2, 0.2),
        "owner": with_ends(jax.random.randint(key_list[3], (DATES,), 0, OWNERS), jax.random.fold_in(key_list[3], 1), 0, OWNERS - 1).astype(jnp.int32),
        "trade_factor": with_ends(jax.random.randint(key_list[4], (TRADES,), 0, F), jax.random.fold_in(key_list[4], 1), 0, F - 1).astype(jnp.int32),
        "trade_set": with_ends(jax.random.randint(key_list[5], (TRADES,), 0, SETS), jax.random.fold_in(key_list[5], 1), 0, SETS - 1).astype(jnp.int32),
        "notional": bell_draw(key_list[6], (TRADES,), 1.0, 5.0, (), jnp.float32),
        "strike": jnp.clip(jax.random.uniform(key_list[7], (TRADES,), jnp.float32, 0.8, 1.25), 0.8, 1.25),
    }


def reference(normal_draws, cholesky, log_spot, owner, trade_factor, trade_set, notional, strike):
    level = jnp.zeros((F, PATHS), jnp.float32) + log_spot[:, None]
    results = []
    for date in range(DATES):
        lower = cholesky[date, owner[date]]
        increment = jnp.dot(lower, normal_draws[date], precision=lax.Precision.HIGHEST, preferred_element_type=jnp.float32)
        level = level + increment
        price = jnp.exp(level)[trade_factor]
        payoff = notional[:, None] * jnp.maximum(price - strike[:, None], 0.0)
        net = jax.ops.segment_sum(payoff, trade_set, num_segments=SETS)
        results.append(jnp.sum(jnp.maximum(net, 0.0), axis=1) / PATHS)
    return jnp.stack(results, axis=0)
```

```python
import jax
import jax.numpy as jnp
from jax import lax
from jax.sharding import PartitionSpec as P

SETS = 512


def carried_in(part, axis, combine, identity):
    place = lax.axis_index(axis)
    gathered = lax.all_gather(part, axis)
    state = jnp.zeros_like(part) + jnp.asarray(identity, part.dtype)

    def one(step, state):
        return combine(state, lax.dynamic_index_in_dim(gathered, step, 0, False))

    return lax.fori_loop(0, place, one, state)


def summed(part, axis):
    size = lax.axis_size(axis)
    if size & (size - 1):
        return lax.psum(part, axis)
    distance = 1
    while distance < size:
        part = part + lax.ppermute(part, axis, [(i, i ^ distance) for i in range(size)])
        distance *= 2
    return part


def add_pair(earlier, later):
    return earlier + later


def shards(normal_draws, cholesky, log_spot, owner, trade_factor, trade_set, notional, strike):
    local_dates = normal_draws.shape[0]
    section_index = lax.axis_index("section")
    owners_here = lax.dynamic_slice_in_dim(owner, section_index * local_dates, local_dates)
    holder = lax.axis_index("paths")
    mine = (owners_here == holder)[:, None, None]
    blocks = summed(jnp.where(mine, cholesky[:, 0], 0.0), "paths")
    lowers = [blocks[date] for date in range(local_dates)]
    running = jnp.zeros(normal_draws.shape[1:], jnp.float32)
    prefixes = []
    for date in range(local_dates):
        increment = jnp.dot(
            lowers[date],
            normal_draws[date],
            precision=lax.Precision.HIGHEST,
            preferred_element_type=jnp.float32,
        )
        running = running + increment
        prefixes.append(running)
    before = carried_in(running, "section", add_pair, jnp.zeros_like(running))
    factor_table = (trade_factor[:, None] == jnp.arange(normal_draws.shape[1])[None, :]).astype(
        jnp.float32
    )
    set_table = (jnp.arange(SETS)[:, None] == trade_set[None, :]).astype(jnp.float32)
    sums = []
    for date in range(local_dates):
        level = log_spot[:, None] + before + prefixes[date]
        price = jnp.dot(
            factor_table,
            jnp.exp(level),
            precision=lax.Precision.HIGHEST,
            preferred_element_type=jnp.float32,
        )
        payoff = notional[:, None] * jnp.maximum(price - strike[:, None], 0.0)
        net = jnp.dot(
            set_table, payoff, precision=lax.Precision.HIGHEST, preferred_element_type=jnp.float32
        )
        sums.append(jnp.sum(jnp.maximum(net, 0.0), axis=1))
    totals = summed(jnp.stack(sums, axis=0), "paths")
    return totals / (normal_draws.shape[2] * lax.axis_size("paths"))


def solution(mesh):
    placed = (
        P("section", None, "paths"),
        P("section", "paths", None, None),
        P(),
        P(),
        P(),
        P(),
        P(),
        P(),
    )
    return jax.shard_map(
        shards, mesh=mesh, in_specs=placed, out_specs=P("section", None), check_vma=False
    )
```

```python
import functools

import jax
import jax.numpy as jnp
from jax import lax
from jax.experimental import pallas as pl
from jax.experimental.pallas import tpu as pltpu
from jax.sharding import PartitionSpec as P

SETS = 512
LANES = 128
BLOCKS = SETS // LANES
CHUNK = 2 * LANES
ROWS = 32
GROUPS = 16
UNROLL = 4


def summed(part, axis):
    size = lax.axis_size(axis)
    if size & (size - 1):
        return lax.psum(part, axis)
    distance = 1
    while distance < size:
        part = part + lax.ppermute(part, axis, [(i, i ^ distance) for i in range(size)])
        distance *= 2
    return part


def pieces(value):
    first = value.astype(jnp.bfloat16).astype(jnp.float32)
    rest = value - first
    second = rest.astype(jnp.bfloat16).astype(jnp.float32)
    return first, second, rest - second


def dot_last(a, b):
    return lax.dot_general(a, b, (((1,), (1,)), ((), ())), preferred_element_type=jnp.float32)


def iota(shape, dim):
    return lax.broadcasted_iota(jnp.int32, shape, dim)


def table_kernel(
    factor_ref, set_ref, notional_ref, strike_ref,
    index_ref, level_ref, weight_ref, offset_ref, place_ref, count_ref,
    before_ref, base_ref, table_ref,
):
    chunks = factor_ref.shape[0] // 2
    before_ref[...] = (iota((CHUNK, CHUNK), 0) < iota((CHUNK, CHUNK), 1)).astype(jnp.bfloat16)
    base_ref[...] = jnp.zeros_like(base_ref)
    table_ref[...] = jnp.zeros_like(table_ref)
    set_ids = iota((SETS, LANES), 0)
    row_ids = iota((ROWS, LANES), 0).astype(jnp.float32)

    def chunk(step, carry):
        masks, rows = [], []
        for half in range(2):
            masks.append(set_ids == set_ref[pl.ds(2 * step + half, 1), :])
        hot = jnp.concatenate([m.astype(jnp.float32).astype(jnp.bfloat16) for m in masks], axis=1)
        earlier = jnp.dot(hot, before_ref[...], preferred_element_type=jnp.float32)
        base = base_ref[...]
        for half in range(2):
            rank = jnp.sum(
                jnp.where(masks[half], earlier[:, half * LANES : (half + 1) * LANES] + base, 0.0),
                axis=0, keepdims=True,
            )
            here = row_ids == rank
            own = pl.ds(2 * step + half, 1)
            values = (
                (factor_ref[own, :].astype(jnp.float32),)
                + pieces(strike_ref[own, :])
                + pieces(notional_ref[own, :])
            )
            rows.append([jnp.where(here, v, 0.0) for v in values])
        parts = [
            jnp.concatenate([rows[0][i], rows[1][i]], axis=1).astype(jnp.bfloat16)
            for i in range(len(rows[0]))
        ]
        parts.append(jnp.ones((16, CHUNK), jnp.bfloat16))
        table_ref[...] += dot_last(jnp.concatenate(parts, axis=0), hot)
        last = earlier[:, CHUNK - 1 :] + masks[1][:, LANES - 1 :].astype(jnp.float32)
        base_ref[...] = base + jnp.broadcast_to(last, (SETS, LANES))
        return carry

    lax.fori_loop(0, chunks, chunk, 0)
    table = table_ref[...]
    counts = table[7 * ROWS : 7 * ROWS + 1, :]
    base = base_ref[...]
    places = []
    for block in range(BLOCKS):
        own = counts[:, block * LANES : (block + 1) * LANES]
        mine = iota((SETS, LANES), 1) + block * LANES
        ahead = (base > own) | ((base == own) & (set_ids < mine))
        places.append(jnp.sum(jnp.where(ahead, 1.0, 0.0), axis=0, keepdims=True))
    place = jnp.concatenate(places, axis=1)
    moved = (iota((SETS, SETS), 0).astype(jnp.float32) == place).astype(jnp.float32)
    moved = moved.astype(jnp.bfloat16)
    place_ref[...] = moved
    table = dot_last(table[: 7 * ROWS, :].astype(jnp.bfloat16), moved)
    index = table[:ROWS, :].astype(jnp.int32)
    level = table[ROWS : 2 * ROWS] + (table[2 * ROWS : 3 * ROWS] + table[3 * ROWS : 4 * ROWS])
    weight = table[4 * ROWS : 5 * ROWS] + (table[5 * ROWS : 6 * ROWS] + table[6 * ROWS :])
    offset = -jnp.sum(level * weight, axis=0, keepdims=True)
    for block in range(BLOCKS):
        own = slice(block * LANES, (block + 1) * LANES)
        index_ref[pl.ds(block * ROWS, ROWS), :] = index[:, own]
        level_ref[pl.ds(block * ROWS, ROWS), :] = level[:, own]
        weight_ref[pl.ds(block * ROWS, ROWS), :] = weight[:, own]
        offset_ref[pl.ds(block, 1), :] = offset[:, own]
        most = jnp.max(jnp.where(place == float(block * LANES), counts, 0.0))
        count_ref[block] = most.astype(jnp.int32)


def tables(trade_factor, trade_set, notional, strike):
    lines = trade_factor.shape[0] // LANES
    packed = [a.reshape(lines, LANES) for a in (trade_factor, trade_set, notional, strike)]
    vmem = pl.BlockSpec(memory_space=pltpu.VMEM)
    grid_rows = (BLOCKS * ROWS, LANES)
    return pl.pallas_call(
        table_kernel,
        out_shape=(
            jax.ShapeDtypeStruct(grid_rows, jnp.int32),
            jax.ShapeDtypeStruct(grid_rows, jnp.float32),
            jax.ShapeDtypeStruct(grid_rows, jnp.float32),
            jax.ShapeDtypeStruct((BLOCKS, LANES), jnp.float32),
            jax.ShapeDtypeStruct((SETS, SETS), jnp.bfloat16),
            jax.ShapeDtypeStruct((BLOCKS,), jnp.int32),
        ),
        in_specs=[vmem] * 4,
        out_specs=(vmem,) * 5 + (pl.BlockSpec(memory_space=pltpu.SMEM),),
        scratch_shapes=[
            pltpu.VMEM((CHUNK, CHUNK), jnp.bfloat16),
            pltpu.VMEM((SETS, LANES), jnp.float32),
            pltpu.VMEM((7 * ROWS + 16, SETS), jnp.float32),
        ],
        cost_estimate=pl.CostEstimate(
            flops=2 * trade_factor.shape[0] * SETS * 500, transcendentals=0, bytes_accessed=1 << 20
        ),
        name="tables",
    )(*packed)


def picked(values, index):
    numbers = lax.GatherDimensionNumbers(
        offset_dims=(), collapsed_slice_dims=(1,), start_index_map=(1,),
        operand_batching_dims=(0,), start_indices_batching_dims=(0,),
    )
    return lax.gather(
        values, index[..., None], numbers, slice_sizes=(1, 1),
        mode=lax.GatherScatterMode.PROMISE_IN_BOUNDS,
    )


def exposure_kernel(
    count_ref, index_ref, strike_ref, weight_ref, offset_ref, place_ref, spot_ref, carry_ref, own_ref,
    factor_hbm, set_hbm, notional_hbm, strike_hbm,
    out_ref,
    level_ref, price_ref, sum_ref, net_ref, factor_s, set_s, notional_s, strike_s,
):
    dates, factors, paths = own_ref.shape
    half = LANES // 2
    carried = carry_ref[...] + spot_ref[...]
    level_ref[...] = jnp.zeros_like(level_ref)
    for date in range(dates):
        level_ref[pl.ds(date * half, factors), :] = jnp.exp(carried + own_ref[date])
    groups = paths // 8
    price_ref[...] = jnp.transpose(level_ref[...]).reshape(groups, 8, LANES)
    sum_ref[...] = jnp.zeros_like(sum_ref)
    largest = count_ref[0]

    @pl.when(largest <= ROWS)
    def _():
        def some(step, carry):
            values = [price_ref[step * GROUPS + i] for i in range(GROUPS)]
            for block in range(BLOCKS):
                start = jnp.broadcast_to(offset_ref[pl.ds(block, 1), :], (8, LANES))

                def rows(r, nets):
                    for u in range(UNROLL):
                        at = pl.ds(block * ROWS + r * UNROLL + u, 1)
                        index = jnp.broadcast_to(index_ref[at, :], (8, LANES))
                        strike = jnp.broadcast_to(strike_ref[at, :], (8, LANES))
                        weight = jnp.broadcast_to(weight_ref[at, :], (8, LANES))
                        nets = tuple(
                            tuple(
                                net + weight * jnp.maximum(picked(v, index + date * half), strike)
                                for net, v in zip(nets[date], values)
                            )
                            for date in range(dates)
                        )
                    return nets

                nets = lax.fori_loop(
                    0, (count_ref[block] + UNROLL - 1) // UNROLL, rows, ((start,) * GROUPS,) * dates
                )
                for date in range(dates):
                    sum_ref[date, block] += sum(jnp.maximum(net, 0.0) for net in nets[date])
            return carry

        lax.fori_loop(0, groups // GROUPS, some, 0)
        total = jnp.concatenate(
            [
                jnp.concatenate(
                    [jnp.sum(sum_ref[date, block], axis=0, keepdims=True) for block in range(BLOCKS)], axis=1
                )
                for date in range(dates)
            ]
            + [jnp.zeros((16 - dates, SETS), jnp.float32)],
            axis=0,
        )
        place = place_ref[...]
        parts = [jnp.dot(p.astype(jnp.bfloat16), place, preferred_element_type=jnp.float32) for p in pieces(total)]
        out_ref[...] = (parts[0] + (parts[1] + parts[2]))[:dates]

    @pl.when(largest > ROWS)
    def _():
        pltpu.sync_copy(factor_hbm, factor_s)
        pltpu.sync_copy(set_hbm, set_s)
        pltpu.sync_copy(notional_hbm, notional_s)
        pltpu.sync_copy(strike_hbm, strike_s)
        for date in range(dates):
            net_ref[...] = jnp.zeros_like(net_ref)

            def trade(t, carry):
                price = level_ref[pl.ds(factor_s[t] + date * half, 1), :]
                at = pl.ds(set_s[t], 1)
                net_ref[at, :] += notional_s[t] * jnp.maximum(price - strike_s[t], 0.0)
                return carry

            lax.fori_loop(0, factor_s.shape[0], trade, 0)
            ones = jnp.ones((8, paths), jnp.float32)
            out_ref[pl.ds(date, 1), :] = lax.dot_general(
                ones, jnp.maximum(net_ref[...], 0.0), (((1,), (1,)), ((), ())),
                precision=lax.Precision.HIGHEST, preferred_element_type=jnp.float32,
            )[:1]


def exposures(built, log_spot, before, own, trades):
    index, strike, weight, offset, place, count = built
    dates, factors, paths = own.shape
    vmem, hbm = pl.BlockSpec(memory_space=pltpu.VMEM), pl.BlockSpec(memory_space=pl.ANY)
    number = trades[0].shape
    return pl.pallas_call(
        exposure_kernel,
        out_shape=jax.ShapeDtypeStruct((dates, SETS), jnp.float32),
        in_specs=[pl.BlockSpec(memory_space=pltpu.SMEM)] + [vmem] * 8 + [hbm] * 4,
        out_specs=vmem,
        scratch_shapes=[
            pltpu.VMEM((LANES, paths), jnp.float32),
            pltpu.VMEM((paths // 8, 8, LANES), jnp.float32),
            pltpu.VMEM((dates, BLOCKS, 8, LANES), jnp.float32),
            pltpu.VMEM((SETS, paths), jnp.float32),
            pltpu.SMEM(number, jnp.int32),
            pltpu.SMEM(number, jnp.int32),
            pltpu.SMEM(number, jnp.float32),
            pltpu.SMEM(number, jnp.float32),
        ],
        name="exposures",
    )(count, index, strike, weight, offset, place, log_spot[:, None], before, own, *trades)


def shards(normal_draws, cholesky, log_spot, owner, trade_factor, trade_set, notional, strike):
    local_dates = normal_draws.shape[0]
    section, sections = lax.axis_index("section"), lax.axis_size("section")
    trades = (trade_factor, trade_set, notional, strike)
    built = tables(*trades)
    owners_here = lax.dynamic_slice_in_dim(owner, section * local_dates, local_dates)
    mine = (owners_here == lax.axis_index("paths"))[:, None, None]
    blocks = summed(jnp.where(mine, cholesky[:, 0], 0.0), "paths")
    running = jnp.zeros(normal_draws.shape[1:], jnp.float32)
    prefixes = []
    for date in range(local_dates):
        increment = jnp.dot(
            blocks[date],
            normal_draws[date],
            precision=lax.Precision.HIGHEST,
            preferred_element_type=jnp.float32,
        )
        running = running + increment
        prefixes.append(running)
    gathered = lax.all_gather(running, "section")
    earlier = (jnp.arange(sections) < section)[:, None, None]
    before = jnp.sum(jnp.where(earlier, gathered, 0.0), axis=0)
    sums = exposures(built, log_spot, before, jnp.stack(prefixes, axis=0), trades)
    totals = summed(sums, "paths")
    return totals / (normal_draws.shape[2] * lax.axis_size("paths"))


def solution(mesh):
    placed = (P("section", None, "paths"), P("section", "paths", None, None)) + (P(),) * 6
    return jax.shard_map(
        shards, mesh=mesh, in_specs=placed, out_specs=P("section", None), check_vma=False
    )
```

```python
import functools

import jax
import jax.numpy as jnp
from jax import lax
from jax.experimental import pallas as pl
from jax.experimental.pallas import tpu as pltpu
from jax.sharding import PartitionSpec as P

SETS = 512
LANES = 128
LOW = 128.0
BLOCKS = SETS // LANES
CHUNK = 2 * LANES
ROWS = 32
GROUP = 16
UNROLL = 2


def summed(part, axis):
    size = lax.axis_size(axis)
    if size & (size - 1):
        return lax.psum(part, axis)
    distance = 1
    while distance < size:
        part = part + lax.ppermute(part, axis, [(i, i ^ distance) for i in range(size)])
        distance *= 2
    return part


def pieces(value):
    first = value.astype(jnp.bfloat16).astype(jnp.float32)
    rest = value - first
    second = rest.astype(jnp.bfloat16).astype(jnp.float32)
    return first, second, rest - second


def dot_last(a, b):
    return lax.dot_general(a, b, (((1,), (1,)), ((), ())), preferred_element_type=jnp.float32)


def iota(shape, dim):
    return lax.broadcasted_iota(jnp.int32, shape, dim)


def table_kernel(
    factor_ref, set_ref, notional_ref, level_ref,
    index_ref, strike_ref, weight_ref, place_ref, count_ref,
    before_ref, base_ref, table_ref,
):
    chunks = factor_ref.shape[0] // 2
    before_ref[...] = (iota((CHUNK, CHUNK), 0) < iota((CHUNK, CHUNK), 1)).astype(jnp.bfloat16)
    base_ref[...] = jnp.zeros_like(base_ref)
    table_ref[...] = jnp.zeros_like(table_ref)
    set_ids = iota((SETS, LANES), 0)
    row_ids = iota((ROWS, LANES), 0).astype(jnp.float32)

    def chunk(step, carry):
        masks, rows = [], []
        for half in range(2):
            masks.append(set_ids == set_ref[pl.ds(2 * step + half, 1), :])
        hot = jnp.concatenate([m.astype(jnp.float32).astype(jnp.bfloat16) for m in masks], axis=1)
        earlier = jnp.dot(hot, before_ref[...], preferred_element_type=jnp.float32)
        base = base_ref[...]
        for half in range(2):
            rank = jnp.sum(
                jnp.where(masks[half], earlier[:, half * LANES : (half + 1) * LANES] + base, 0.0),
                axis=0, keepdims=True,
            )
            here = row_ids == rank
            own = pl.ds(2 * step + half, 1)
            values = (
                (factor_ref[own, :].astype(jnp.float32),)
                + pieces(level_ref[own, :])
                + pieces(notional_ref[own, :])
            )
            rows.append([jnp.where(here, v, 0.0) for v in values])
        parts = [
            jnp.concatenate([rows[0][i], rows[1][i]], axis=1).astype(jnp.bfloat16)
            for i in range(len(rows[0]))
        ]
        parts.append(jnp.ones((16, CHUNK), jnp.bfloat16))
        table_ref[...] += dot_last(jnp.concatenate(parts, axis=0), hot)
        last = earlier[:, CHUNK - 1 :] + masks[1][:, LANES - 1 :].astype(jnp.float32)
        base_ref[...] = base + jnp.broadcast_to(last, (SETS, LANES))
        return carry

    lax.fori_loop(0, chunks, chunk, 0, unroll=4)
    table = table_ref[...]
    counts = table[7 * ROWS : 7 * ROWS + 1, :]
    base = base_ref[...]
    places = []
    for block in range(BLOCKS):
        own = counts[:, block * LANES : (block + 1) * LANES]
        mine = iota((SETS, LANES), 1) + block * LANES
        ahead = (base > own) | ((base == own) & (set_ids < mine))
        places.append(jnp.sum(jnp.where(ahead, 1.0, 0.0), axis=0, keepdims=True))
    place = jnp.concatenate(places, axis=1)
    moved = (iota((SETS, SETS), 0).astype(jnp.float32) == place).astype(jnp.float32)
    moved = moved.astype(jnp.bfloat16)
    place_ref[...] = moved
    table = dot_last(table[: 7 * ROWS, :].astype(jnp.bfloat16), moved)
    index = table[:ROWS, :].astype(jnp.int32)
    strike = table[ROWS : 2 * ROWS] + (table[2 * ROWS : 3 * ROWS] + table[3 * ROWS : 4 * ROWS])
    weight = table[4 * ROWS : 5 * ROWS] + (table[5 * ROWS : 6 * ROWS] + table[6 * ROWS : 7 * ROWS])
    for block in range(BLOCKS):
        own = slice(block * LANES, (block + 1) * LANES)
        index_ref[:, block, :] = index[:, own]
        strike_ref[:, block, :] = strike[:, own]
        weight_ref[:, block, :] = weight[:, own]
    exact = jnp.concatenate([(counts - LOW * jnp.floor(counts / LOW)), jnp.floor(counts / LOW)] + [jnp.zeros((14, SETS), jnp.float32)], axis=0)
    ordered = dot_last(exact.astype(jnp.bfloat16), moved)
    count_ref[...] = (ordered[:1] + LOW * ordered[1:2]).astype(jnp.int32)


def tables(trade_factor, trade_set, notional, strike):
    lines = trade_factor.shape[0] // LANES
    packed = [a.reshape(lines, LANES) for a in (trade_factor, trade_set, notional, strike)]
    vmem = pl.BlockSpec(memory_space=pltpu.VMEM)
    grid_rows = (ROWS, BLOCKS, LANES)
    return pl.pallas_call(
        table_kernel,
        out_shape=(
            jax.ShapeDtypeStruct(grid_rows, jnp.int32),
            jax.ShapeDtypeStruct(grid_rows, jnp.float32),
            jax.ShapeDtypeStruct(grid_rows, jnp.float32),
            jax.ShapeDtypeStruct((SETS, SETS), jnp.bfloat16),
            jax.ShapeDtypeStruct((1, SETS), jnp.int32),
        ),
        in_specs=[vmem] * 4,
        out_specs=(vmem,) * 5,
        scratch_shapes=[
            pltpu.VMEM((CHUNK, CHUNK), jnp.bfloat16),
            pltpu.VMEM((SETS, LANES), jnp.float32),
            pltpu.VMEM((7 * ROWS + 16, SETS), jnp.float32),
        ],
        cost_estimate=pl.CostEstimate(
            flops=2 * trade_factor.shape[0] * SETS * 500, transcendentals=0, bytes_accessed=1 << 20
        ),
        name="tables",
    )(*packed)


def over_sublanes(nets):
    row = iota((8, LANES), 0)
    for bit in (4, 2, 1):
        low = (row & bit) == 0
        nets = [
            jnp.where(low, a, pltpu.roll(b, bit, 0)) + jnp.where(low, pltpu.roll(a, 8 - bit, 0), b)
            for a, b in zip(nets[: len(nets) // 2], nets[len(nets) // 2 :])
        ]
    return nets[0]


def exposure_kernel(
    count_ref, index_ref, strike_ref, weight_ref, place_ref, spot_ref, carry_ref, own_ref,
    factor_hbm, set_hbm, notional_hbm, strike_hbm,
    out_ref,
    level_ref, price_ref, sum_ref, net_ref, factor_s, set_s, notional_s, strike_s,
):
    dates, factors, paths = own_ref.shape
    tiles = paths // LANES
    carried = carry_ref[...] + spot_ref[...]
    for date in range(dates):
        level = jnp.exp(carried + own_ref[date])
        level_ref[date] = level
        price_ref[:, date] = level.reshape(factors, tiles, LANES)
    largest = count_ref[0]

    @pl.when(largest <= ROWS)
    def _():
        def group(step, carry):
            first = step * GROUP

            def rows(r, nets):
                nets = [list(n) for n in nets]
                base = r * (UNROLL * SETS) + first
                for u in range(UNROLL):
                    for j in range(GROUP):
                        slot = base + u * SETS + j
                        index, strike, weight = index_ref[slot], strike_ref[slot], weight_ref[slot]
                        for date in range(dates):
                            price = price_ref[index, date]
                            nets[date][j] += weight * jnp.maximum(price - strike, 0.0)
                return tuple(tuple(n) for n in nets)

            zero = jnp.zeros((tiles, LANES), jnp.float32)
            nets = lax.fori_loop(
                0, (count_ref[first] + UNROLL - 1) // UNROLL, rows, ((zero,) * GROUP,) * dates
            )
            for date in range(dates):
                for part in range(GROUP // 8):
                    eight = [jnp.maximum(nets[date][part * 8 + i], 0.0) for i in range(8)]
                    at = pl.ds(pl.multiple_of(first + part * 8, 8), 8)
                    sum_ref[date, at, :] = over_sublanes(eight)
            return carry

        lax.fori_loop(0, SETS // GROUP, group, 0)
        ones = jnp.ones((8, LANES), jnp.bfloat16)
        lines = []
        for date in range(dates):
            lines.append(sum(dot_last(ones, p.astype(jnp.bfloat16)) for p in pieces(sum_ref[date]))[:1])
        total = jnp.concatenate(lines + [jnp.zeros((16 - dates, SETS), jnp.float32)], axis=0)
        place = place_ref[...]
        parts = [jnp.dot(p.astype(jnp.bfloat16), place, preferred_element_type=jnp.float32) for p in pieces(total)]
        out_ref[...] = (parts[0] + (parts[1] + parts[2]))[:dates]

    @pl.when(largest > ROWS)
    def _():
        pltpu.sync_copy(factor_hbm, factor_s)
        pltpu.sync_copy(set_hbm, set_s)
        pltpu.sync_copy(notional_hbm, notional_s)
        pltpu.sync_copy(strike_hbm, strike_s)

        def one_date(date, carry):
            net_ref[...] = jnp.zeros_like(net_ref)

            def trade(t, carry):
                price = level_ref[date, pl.ds(factor_s[t], 1), :]
                at = pl.ds(set_s[t], 1)
                net_ref[at, :] += notional_s[t] * jnp.maximum(price - strike_s[t], 0.0)
                return carry

            lax.fori_loop(0, factor_s.shape[0], trade, 0)
            sums = jnp.zeros((8, SETS), jnp.float32)
            ones = jnp.ones((8, LANES), jnp.bfloat16)
            for tile in range(tiles):
                for p in pieces(jnp.maximum(net_ref[:, tile * LANES : (tile + 1) * LANES], 0.0)):
                    sums += dot_last(ones, p.astype(jnp.bfloat16))
            out_ref[pl.ds(date, 1), :] = sums[:1]
            return carry

        lax.fori_loop(0, dates, one_date, 0)


def exposures(built, log_spot, before, own, trades):
    index, strike, weight, place, count = built
    dates, factors, paths = own.shape
    vmem, hbm = pl.BlockSpec(memory_space=pltpu.VMEM), pl.BlockSpec(memory_space=pl.ANY)
    number = trades[0].shape
    return pl.pallas_call(
        exposure_kernel,
        out_shape=jax.ShapeDtypeStruct((dates, SETS), jnp.float32),
        in_specs=[pl.BlockSpec(memory_space=pltpu.SMEM)] * 4 + [vmem] * 4 + [hbm] * 4,
        out_specs=vmem,
        scratch_shapes=[
            pltpu.VMEM((dates, factors, paths), jnp.float32),
            pltpu.VMEM((factors, dates, paths // LANES, LANES), jnp.float32),
            pltpu.VMEM((dates, SETS, LANES), jnp.float32),
            pltpu.VMEM((SETS, paths), jnp.float32),
            pltpu.SMEM(number, jnp.int32),
            pltpu.SMEM(number, jnp.int32),
            pltpu.SMEM(number, jnp.float32),
            pltpu.SMEM(number, jnp.float32),
        ],
        name="exposures",
    )(count.reshape(SETS), index.reshape(-1), strike.reshape(-1), weight.reshape(-1), place, log_spot[:, None], before, own, *trades)


def shards(normal_draws, cholesky, log_spot, owner, trade_factor, trade_set, notional, strike):
    local_dates = normal_draws.shape[0]
    section, sections = lax.axis_index("section"), lax.axis_size("section")
    trades = (trade_factor, trade_set, notional, strike)
    built = tables(*trades)
    owners_here = lax.dynamic_slice_in_dim(owner, section * local_dates, local_dates)
    mine = (owners_here == lax.axis_index("paths"))[:, None, None]
    blocks = summed(jnp.where(mine, cholesky[:, 0], 0.0), "paths")
    running = jnp.zeros(normal_draws.shape[1:], jnp.float32)
    prefixes = []
    for date in range(local_dates):
        increment = jnp.dot(
            blocks[date],
            normal_draws[date],
            precision=lax.Precision.HIGHEST,
            preferred_element_type=jnp.float32,
        )
        running = running + increment
        prefixes.append(running)
    gathered = lax.all_gather(running, "section")
    earlier = (jnp.arange(sections) < section)[:, None, None]
    before = jnp.sum(jnp.where(earlier, gathered, 0.0), axis=0)
    sums = exposures(built, log_spot, before, jnp.stack(prefixes, axis=0), trades)
    totals = summed(sums, "paths")
    return totals / (normal_draws.shape[2] * lax.axis_size("paths"))


def solution(mesh):
    placed = (P("section", None, "paths"), P("section", "paths", None, None)) + (P(),) * 6
    return jax.shard_map(
        shards, mesh=mesh, in_specs=placed, out_specs=P("section", None), check_vma=False
    )
```

```python
import functools

import jax
import jax.numpy as jnp
from jax import lax
from jax.experimental import pallas as pl
from jax.experimental.pallas import tpu as pltpu
from jax.sharding import PartitionSpec as P

SETS = 512
LANES = 128
LOW = 128.0
BLOCKS = SETS // LANES
CHUNK = 2 * LANES
ROWS = 32
PAIRS = ROWS // 2
SHIFT = 16
GROUP = 16
PARTS = 4


def summed(part, axis):
    size = lax.axis_size(axis)
    if size & (size - 1):
        return lax.psum(part, axis)
    distance = 1
    while distance < size:
        part = part + lax.ppermute(part, axis, [(i, i ^ distance) for i in range(size)])
        distance *= 2
    return part


def pieces(value):
    first = value.astype(jnp.bfloat16).astype(jnp.float32)
    rest = value - first
    second = rest.astype(jnp.bfloat16).astype(jnp.float32)
    return first, second, rest - second


def dot_last(a, b):
    return lax.dot_general(a, b, (((1,), (1,)), ((), ())), preferred_element_type=jnp.float32)


def iota(shape, dim):
    return lax.broadcasted_iota(jnp.int32, shape, dim)


def moves(place):
    hot = iota((SETS, SETS), 0).astype(jnp.float32) == place
    return hot.astype(jnp.float32).astype(jnp.bfloat16)


def table_kernel(
    step, factor_ref, set_ref, notional_ref, level_ref,
    index_ref, strike_ref, weight_ref, place_ref, count_ref,
    before_ref, base_ref, table_ref,
):
    chunks = factor_ref.shape[0] // 2
    before_ref[...] = (iota((CHUNK, CHUNK), 0) < iota((CHUNK, CHUNK), 1)).astype(jnp.bfloat16)
    base_ref[...] = jnp.zeros_like(base_ref)
    table_ref[...] = jnp.zeros_like(table_ref)
    set_ids = iota((SETS, LANES), 0)
    rows_at = iota((ROWS, LANES), 0)
    row_ids = jnp.where(rows_at < PAIRS, 2 * rows_at, 2 * (rows_at - PAIRS) + 1).astype(jnp.float32)

    def chunk(turn, carry):
        masks, rows = [], []
        for half in range(2):
            masks.append(set_ids == set_ref[pl.ds(2 * turn + half, 1), :])
        hot = jnp.concatenate([m.astype(jnp.float32).astype(jnp.bfloat16) for m in masks], axis=1)
        earlier = jnp.dot(hot, before_ref[...], preferred_element_type=jnp.float32)
        base = base_ref[...]
        for half in range(2):
            rank = jnp.sum(
                jnp.where(masks[half], earlier[:, half * LANES : (half + 1) * LANES] + base, 0.0),
                axis=0, keepdims=True,
            )
            here = row_ids == rank
            own = pl.ds(2 * turn + half, 1)
            values = (
                (factor_ref[own, :].astype(jnp.float32),)
                + pieces(level_ref[own, :])
                + pieces(notional_ref[own, :])
            )
            rows.append([jnp.where(here, v, 0.0) for v in values])
        parts = [
            jnp.concatenate([rows[0][i], rows[1][i]], axis=1).astype(jnp.bfloat16)
            for i in range(len(rows[0]))
        ]
        parts.append(jnp.ones((16, CHUNK), jnp.bfloat16))
        table_ref[...] += dot_last(jnp.concatenate(parts, axis=0), hot)
        last = earlier[:, CHUNK - 1 :] + masks[1][:, LANES - 1 :].astype(jnp.float32)
        base_ref[...] = base + jnp.broadcast_to(last, (SETS, LANES))
        return carry

    lax.fori_loop(0, chunks, chunk, 0, unroll=4)
    table = table_ref[...]
    counts = table[7 * ROWS : 7 * ROWS + 1, :]
    base = base_ref[...]
    places = []
    for block in range(BLOCKS):
        own = counts[:, block * LANES : (block + 1) * LANES]
        mine = iota((SETS, LANES), 1) + block * LANES
        ahead = (base > own) | ((base == own) & (set_ids < mine))
        places.append(jnp.sum(jnp.where(ahead, 1.0, 0.0), axis=0, keepdims=True))
    place = jnp.concatenate(places, axis=1)
    moved = moves(place)
    place_ref[...] = place
    table = dot_last(table[: 7 * ROWS, :].astype(jnp.bfloat16), moved)
    index = table[:ROWS, :].astype(jnp.int32)
    index = (index[:PAIRS] + (index[PAIRS:] << SHIFT)) * step
    strike = table[ROWS : 2 * ROWS] + (table[2 * ROWS : 3 * ROWS] + table[3 * ROWS : 4 * ROWS])
    weight = table[4 * ROWS : 5 * ROWS] + (table[5 * ROWS : 6 * ROWS] + table[6 * ROWS : 7 * ROWS])
    for block in range(BLOCKS):
        own = slice(block * LANES, (block + 1) * LANES)
        index_ref[:, block, :] = index[:, own]
        for half in range(2):
            at = slice(half * PAIRS, (half + 1) * PAIRS)
            strike_ref[:, half * BLOCKS + block, :] = strike[at, own]
            weight_ref[:, half * BLOCKS + block, :] = weight[at, own]
    exact = jnp.concatenate([(counts - LOW * jnp.floor(counts / LOW)), jnp.floor(counts / LOW)] + [jnp.zeros((14, SETS), jnp.float32)], axis=0)
    ordered = dot_last(exact.astype(jnp.bfloat16), moved)
    count_ref[...] = (ordered[:1] + LOW * ordered[1:2]).astype(jnp.int32)


def tables(step, trade_factor, trade_set, notional, strike):
    lines = trade_factor.shape[0] // LANES
    packed = [a.reshape(lines, LANES) for a in (trade_factor, trade_set, notional, strike)]
    vmem = pl.BlockSpec(memory_space=pltpu.VMEM)
    return pl.pallas_call(
        functools.partial(table_kernel, step),
        out_shape=(
            jax.ShapeDtypeStruct((PAIRS, BLOCKS, LANES), jnp.int32),
            jax.ShapeDtypeStruct((PAIRS, 2 * BLOCKS, LANES), jnp.float32),
            jax.ShapeDtypeStruct((PAIRS, 2 * BLOCKS, LANES), jnp.float32),
            jax.ShapeDtypeStruct((1, SETS), jnp.float32),
            jax.ShapeDtypeStruct((1, SETS), jnp.int32),
        ),
        in_specs=[vmem] * 4,
        out_specs=(vmem,) * 5,
        scratch_shapes=[
            pltpu.VMEM((CHUNK, CHUNK), jnp.bfloat16),
            pltpu.VMEM((SETS, LANES), jnp.float32),
            pltpu.VMEM((7 * ROWS + 16, SETS), jnp.float32),
        ],
        cost_estimate=pl.CostEstimate(
            flops=2 * trade_factor.shape[0] * SETS * 500, transcendentals=0, bytes_accessed=1 << 20
        ),
        compiler_params=pltpu.CompilerParams(vmem_limit_bytes=8 << 20),
        name="tables",
    )(*packed)


def over_sublanes(nets):
    row = iota((8, LANES), 0)
    for bit in (4, 2, 1):
        low = (row & bit) == 0
        nets = [
            jnp.where(low, a, pltpu.roll(b, bit, 0)) + jnp.where(low, pltpu.roll(a, 8 - bit, 0), b)
            for a, b in zip(nets[: len(nets) // 2], nets[len(nets) // 2 :])
        ]
    return nets[0]


def exposure_kernel(
    count_ref, index_hbm, level_hbm, weight_hbm, place_ref, carry_ref, first_ref, second_ref,
    factor_hbm, set_hbm, notional_hbm, strike_hbm,
    out_ref,
    index_ref, limit_ref, weight_ref, copied, level_ref, price_ref, sum_ref, net_ref, factor_s, set_s, notional_s, strike_s,
):
    own_refs = (first_ref, second_ref)
    dates, (factors, paths) = len(own_refs), first_ref.shape
    tiles = paths // LANES
    largest = count_ref[0]
    fits = largest <= ROWS
    copies = []
    for part in range(PARTS):
        each = PAIRS // PARTS
        wanted = fits & ((largest > 2 * each * part) | (part == 0))
        both = []
        for source, target, row in ((index_hbm, index_ref, SETS), (level_hbm, limit_ref, 2 * SETS), (weight_hbm, weight_ref, 2 * SETS)):
            at = pl.ds(part * each * row, each * row)
            both.append(pltpu.make_async_copy(source.at[at], target.at[at], copied.at[part, len(both)]))
        copies.append((wanted, both))

        @pl.when(wanted)
        def _(both=both):
            for copy in both:
                copy.start()

    stacked_ref = price_ref.reshape(factors, dates, tiles, LANES)
    carried = carry_ref[...]
    for date in range(dates):
        level = jnp.exp(carried + own_refs[date][...])
        level_ref[date] = level
        stacked_ref[:, date] = level.reshape(factors, tiles, LANES)

    @pl.when(fits)
    def _():
        def group(step, carry):
            first = (SETS // GROUP - 1 - step) * GROUP
            count = count_ref[first]
            smaller = jnp.where(step == 0, -1, count_ref[jnp.minimum(first + GROUP, SETS - 1)])
            for part, (_, both) in enumerate(copies):
                needed = 2 * (PAIRS // PARTS) * part if part else -1

                @pl.when((count > needed) & (smaller <= needed))
                def _(both=both):
                    for copy in both:
                        copy.wait()

            def rows(r, nets):
                nets = [list(n) for n in nets]
                packs = index_ref.at[pl.ds(r * SETS + first, GROUP)]
                for u in range(2):
                    at = pl.ds(r * (2 * SETS) + u * SETS + first, GROUP)
                    strikes, weights = limit_ref.at[at], weight_ref.at[at]
                    for j in range(GROUP):
                        index = packs[j] >> SHIFT if u else packs[j] & ((1 << SHIFT) - 1)
                        strike, weight = strikes[j], weights[j]
                        for date in range(dates):
                            price = price_ref[pl.ds(pl.multiple_of(index + date * tiles, 8), tiles), :]
                            nets[date][j] += weight * jnp.maximum(price - strike, 0.0)
                return tuple(tuple(n) for n in nets)

            zero = jnp.zeros((tiles, LANES), jnp.float32)
            nets = lax.fori_loop(
                0, (count + 1) // 2, rows, ((zero,) * GROUP,) * dates
            )
            for date in range(dates):
                for part in range(GROUP // 8):
                    eight = [jnp.maximum(nets[date][part * 8 + i], 0.0) for i in range(8)]
                    at = pl.ds(pl.multiple_of(first + part * 8, 8), 8)
                    sum_ref[date, at, :] = over_sublanes(eight)
            return carry

        lax.fori_loop(0, SETS // GROUP, group, 0)
        ones = jnp.ones((8, LANES), jnp.bfloat16)
        lines = []
        for date in range(dates):
            lines.append(sum(dot_last(ones, p.astype(jnp.bfloat16)) for p in pieces(sum_ref[date]))[:1])
        total = jnp.concatenate(lines + [jnp.zeros((16 - dates, SETS), jnp.float32)], axis=0)
        moved = moves(place_ref[...])
        parts = [jnp.dot(p.astype(jnp.bfloat16), moved, preferred_element_type=jnp.float32) for p in pieces(total)]
        out_ref[...] = (parts[0] + (parts[1] + parts[2]))[:dates]

    @pl.when(largest > ROWS)
    def _():
        pltpu.sync_copy(factor_hbm, factor_s)
        pltpu.sync_copy(set_hbm, set_s)
        pltpu.sync_copy(notional_hbm, notional_s)
        pltpu.sync_copy(strike_hbm, strike_s)

        def one_date(date, carry):
            net_ref[...] = jnp.zeros_like(net_ref)

            def trade(t, carry):
                price = level_ref[date, pl.ds(factor_s[t], 1), :]
                at = pl.ds(set_s[t], 1)
                net_ref[at, :] += notional_s[t] * jnp.maximum(price - strike_s[t], 0.0)
                return carry

            lax.fori_loop(0, factor_s.shape[0], trade, 0)
            sums = jnp.zeros((8, SETS), jnp.float32)
            ones = jnp.ones((8, LANES), jnp.bfloat16)
            for tile in range(tiles):
                for p in pieces(jnp.maximum(net_ref[:, tile * LANES : (tile + 1) * LANES], 0.0)):
                    sums += dot_last(ones, p.astype(jnp.bfloat16))
            out_ref[pl.ds(date, 1), :] = sums[:1]
            return carry

        lax.fori_loop(0, dates, one_date, 0)


def exposures(built, before, first, second, trades):
    index, level, weight, place, count = built
    dates, (factors, paths) = 2, first.shape
    vmem, hbm = pl.BlockSpec(memory_space=pltpu.VMEM), pl.BlockSpec(memory_space=pl.ANY)
    number = trades[0].shape
    return pl.pallas_call(
        exposure_kernel,
        out_shape=jax.ShapeDtypeStruct((dates, SETS), jnp.float32),
        in_specs=[pl.BlockSpec(memory_space=pltpu.SMEM)] + [hbm] * 3 + [vmem] * 4 + [hbm] * 4,
        out_specs=vmem,
        scratch_shapes=[
            pltpu.SMEM((PAIRS * SETS,), jnp.int32),
            pltpu.SMEM((PAIRS * 2 * SETS,), jnp.float32),
            pltpu.SMEM((PAIRS * 2 * SETS,), jnp.float32),
            pltpu.SemaphoreType.DMA((PARTS, 3)),
            pltpu.VMEM((dates, factors, paths), jnp.float32),
            pltpu.VMEM((factors * dates * (paths // LANES), LANES), jnp.float32),
            pltpu.VMEM((dates, SETS, LANES), jnp.float32),
            pltpu.VMEM((SETS, paths), jnp.float32),
            pltpu.SMEM(number, jnp.int32),
            pltpu.SMEM(number, jnp.int32),
            pltpu.SMEM(number, jnp.float32),
            pltpu.SMEM(number, jnp.float32),
        ],
        compiler_params=pltpu.CompilerParams(vmem_limit_bytes=12 << 20),
        name="exposures",
    )(count.reshape(SETS), index.reshape(-1), level.reshape(-1), weight.reshape(-1), place, before, first, second, *trades)


def carried_in(total, fill):
    sections, section = lax.axis_size("section"), lax.axis_index("section")
    before = jnp.zeros_like(total)
    middle = total.shape[1] // 2
    odd = (section & 1) == 1
    distance, filled = 1, None
    while distance < sections:
        last = 2 * distance == sections
        pairs = [(i, i ^ distance) for i in range(sections) if not (last and i & distance)]
        if distance == 1:
            got = lax.ppermute(total, "section", pairs)
        else:
            half = jnp.where(odd, total[:, middle:], total[:, :middle])
            if filled is None:
                half, filled = fill(half)
            own = lax.ppermute(half, "section", pairs)
            own, filled = lax.optimization_barrier((own, filled))
            other = lax.ppermute(own, "section", [(i, i ^ 1) for i in range(sections)])
            got = jnp.concatenate([jnp.where(odd, other, own), jnp.where(odd, own, other)], axis=1)
        before = before + jnp.where((section & distance) != 0, got, 0.0)
        if not last:
            total = total + got
        distance *= 2
    return before, fill(total)[1] if filled is None else filled


def shards(normal_draws, cholesky, log_spot, owner, trade_factor, trade_set, notional, strike):
    dates, factors, paths = normal_draws.shape
    half = LANES // 2
    section = lax.axis_index("section")
    trades = (trade_factor, trade_set, notional, strike)
    owners_here = lax.dynamic_slice_in_dim(owner, section * dates, dates)
    mine = owners_here == lax.axis_index("paths")
    spare = ((0, 0), (0, half - factors))
    packed = [jnp.pad(jnp.where(mine[d], cholesky[d, 0], 0.0), spare) for d in range(dates)]
    blocks = summed(jnp.concatenate(packed, axis=1), "paths")
    draws = jnp.pad(normal_draws, ((0, 0), (0, half - factors), (0, 0))).reshape(dates * half, paths)
    first, second = (
        jnp.dot(
            blocks[:, : (date + 1) * half],
            draws[: (date + 1) * half],
            precision=lax.Precision.HIGHEST,
            preferred_element_type=jnp.float32,
        )
        for date in range(dates)
    )

    def fill(ready, first=first):
        ready, own, tied = lax.optimization_barrier((ready, first, trades))
        return ready, (own, tables(dates * paths // LANES, *tied))

    before, (first, built) = carried_in(second, fill)
    sums = exposures(built, before + log_spot[:, None], first, second, trades)
    totals = summed(sums, "paths")
    return totals / (paths * lax.axis_size("paths"))


def solution(mesh):
    placed = (P("section", None, "paths"), P("section", "paths", None, None)) + (P(),) * 6
    return jax.shard_map(
        shards, mesh=mesh, in_specs=placed, out_specs=P("section", None), check_vma=False
    )
```

```python
import functools

import jax
import jax.numpy as jnp
from jax import lax
from jax.experimental import pallas as pl
from jax.experimental.pallas import tpu as pltpu
from jax.sharding import PartitionSpec as P

SETS = 512
LANES = 128
LOW = 128.0
BLOCKS = SETS // LANES
CHUNK = 2 * LANES
ROWS = 32
PAIRS = ROWS // 2
SHIFT = 16
GROUP = 16
PARTS = 8


def summed(part, axis):
    size = lax.axis_size(axis)
    if size & (size - 1):
        return lax.psum(part, axis)
    distance = 1
    while distance < size:
        part = part + lax.ppermute(part, axis, [(i, i ^ distance) for i in range(size)])
        distance *= 2
    return part


def pieces(value):
    first = value.astype(jnp.bfloat16).astype(jnp.float32)
    rest = value - first
    second = rest.astype(jnp.bfloat16).astype(jnp.float32)
    return first, second, rest - second


def dot_last(a, b):
    return lax.dot_general(a, b, (((1,), (1,)), ((), ())), preferred_element_type=jnp.float32)


def iota(shape, dim):
    return lax.broadcasted_iota(jnp.int32, shape, dim)


def moves(place):
    hot = iota((SETS, SETS), 0).astype(jnp.float32) == place
    return hot.astype(jnp.float32).astype(jnp.bfloat16)


def table_kernel(
    step, factor_ref, set_ref, notional_ref, level_ref,
    index_ref, strike_ref, weight_ref, place_ref, count_ref,
    before_ref, base_ref, table_ref,
):
    chunks = factor_ref.shape[0] // 2
    before_ref[...] = (iota((CHUNK, CHUNK), 0) < iota((CHUNK, CHUNK), 1)).astype(jnp.bfloat16)
    base_ref[...] = jnp.zeros_like(base_ref)
    table_ref[...] = jnp.zeros_like(table_ref)
    set_ids = iota((SETS, LANES), 0)
    rows_at = iota((ROWS, LANES), 0)
    row_ids = jnp.where(rows_at < PAIRS, 2 * rows_at, 2 * (rows_at - PAIRS) + 1).astype(jnp.float32)

    def chunk(turn, carry):
        masks, rows = [], []
        for half in range(2):
            masks.append(set_ids == set_ref[pl.ds(2 * turn + half, 1), :])
        hot = jnp.concatenate([m.astype(jnp.float32).astype(jnp.bfloat16) for m in masks], axis=1)
        earlier = jnp.dot(hot, before_ref[...], preferred_element_type=jnp.float32)
        base = base_ref[...]
        for half in range(2):
            rank = jnp.sum(
                jnp.where(masks[half], earlier[:, half * LANES : (half + 1) * LANES] + base, 0.0),
                axis=0, keepdims=True,
            )
            here = row_ids == rank
            own = pl.ds(2 * turn + half, 1)
            values = (
                (factor_ref[own, :].astype(jnp.float32),)
                + pieces(level_ref[own, :])
                + pieces(notional_ref[own, :])
            )
            rows.append([jnp.where(here, v, 0.0) for v in values])
        parts = [
            jnp.concatenate([rows[0][i], rows[1][i]], axis=1).astype(jnp.bfloat16)
            for i in range(len(rows[0]))
        ]
        parts.append(jnp.ones((16, CHUNK), jnp.bfloat16))
        table_ref[...] += dot_last(jnp.concatenate(parts, axis=0), hot)
        last = earlier[:, CHUNK - 1 :] + masks[1][:, LANES - 1 :].astype(jnp.float32)
        base_ref[...] = base + jnp.broadcast_to(last, (SETS, LANES))
        return carry

    lax.fori_loop(0, chunks, chunk, 0, unroll=4)
    table = table_ref[...]
    counts = table[7 * ROWS : 7 * ROWS + 1, :]
    base = base_ref[...]
    places = []
    for block in range(BLOCKS):
        own = counts[:, block * LANES : (block + 1) * LANES]
        mine = iota((SETS, LANES), 1) + block * LANES
        ahead = (base > own) | ((base == own) & (set_ids < mine))
        places.append(jnp.sum(jnp.where(ahead, 1.0, 0.0), axis=0, keepdims=True))
    place = jnp.concatenate(places, axis=1)
    moved = moves(place)
    place_ref[...] = place
    table = dot_last(table[: 7 * ROWS, :].astype(jnp.bfloat16), moved)
    index = table[:ROWS, :].astype(jnp.int32)
    index = (index[:PAIRS] + (index[PAIRS:] << SHIFT)) * step
    strike = table[ROWS : 2 * ROWS] + (table[2 * ROWS : 3 * ROWS] + table[3 * ROWS : 4 * ROWS])
    weight = table[4 * ROWS : 5 * ROWS] + (table[5 * ROWS : 6 * ROWS] + table[6 * ROWS : 7 * ROWS])
    for block in range(BLOCKS):
        own = slice(block * LANES, (block + 1) * LANES)
        index_ref[:, block, :] = index[:, own]
        for half in range(2):
            at = slice(half * PAIRS, (half + 1) * PAIRS)
            strike_ref[:, half * BLOCKS + block, :] = strike[at, own]
            weight_ref[:, half * BLOCKS + block, :] = weight[at, own]
    exact = jnp.concatenate([(counts - LOW * jnp.floor(counts / LOW)), jnp.floor(counts / LOW)] + [jnp.zeros((14, SETS), jnp.float32)], axis=0)
    ordered = dot_last(exact.astype(jnp.bfloat16), moved)
    count_ref[...] = (ordered[:1] + LOW * ordered[1:2]).astype(jnp.int32)


def tables(step, trade_factor, trade_set, notional, strike):
    lines = trade_factor.shape[0] // LANES
    packed = [a.reshape(lines, LANES) for a in (trade_factor, trade_set, notional, strike)]
    vmem = pl.BlockSpec(memory_space=pltpu.VMEM)
    return pl.pallas_call(
        functools.partial(table_kernel, step),
        out_shape=(
            jax.ShapeDtypeStruct((PAIRS, BLOCKS, LANES), jnp.int32),
            jax.ShapeDtypeStruct((PAIRS, 2 * BLOCKS, LANES), jnp.float32),
            jax.ShapeDtypeStruct((PAIRS, 2 * BLOCKS, LANES), jnp.float32),
            jax.ShapeDtypeStruct((1, SETS), jnp.float32),
            jax.ShapeDtypeStruct((1, SETS), jnp.int32),
        ),
        in_specs=[vmem] * 4,
        out_specs=(vmem,) * 5,
        scratch_shapes=[
            pltpu.VMEM((CHUNK, CHUNK), jnp.bfloat16),
            pltpu.VMEM((SETS, LANES), jnp.float32),
            pltpu.VMEM((7 * ROWS + 16, SETS), jnp.float32),
        ],
        cost_estimate=pl.CostEstimate(
            flops=2 * trade_factor.shape[0] * SETS * 500, transcendentals=0, bytes_accessed=1 << 20
        ),
        compiler_params=pltpu.CompilerParams(vmem_limit_bytes=8 << 20),
        name="tables",
    )(*packed)


def over_sublanes(nets):
    row = iota((8, LANES), 0)
    for bit in (4, 2, 1):
        low = (row & bit) == 0
        nets = [
            jnp.where(low, a, pltpu.roll(b, bit, 0)) + jnp.where(low, pltpu.roll(a, 8 - bit, 0), b)
            for a, b in zip(nets[: len(nets) // 2], nets[len(nets) // 2 :])
        ]
    return nets[0]


def exposure_kernel(
    count_ref, index_hbm, level_hbm, weight_hbm, place_ref, carry_ref, first_ref, second_ref,
    factor_hbm, set_hbm, notional_hbm, strike_hbm,
    out_ref,
    index_ref, limit_ref, weight_ref, copied, level_ref, price_ref, sum_ref, net_ref, factor_s, set_s, notional_s, strike_s,
):
    own_refs = (first_ref, second_ref)
    dates, (factors, paths) = len(own_refs), first_ref.shape
    tiles = paths // LANES
    largest = count_ref[0]
    fits = largest <= ROWS
    copies = []
    for part in range(PARTS):
        each = PAIRS // PARTS
        wanted = fits & ((largest > 2 * each * part) | (part == 0))
        both = []
        for source, target, row in ((index_hbm, index_ref, SETS), (level_hbm, limit_ref, 2 * SETS), (weight_hbm, weight_ref, 2 * SETS)):
            at = pl.ds(part * each * row, each * row)
            both.append(pltpu.make_async_copy(source.at[at], target.at[at], copied.at[part, len(both)]))
        copies.append((wanted, both))

        @pl.when(wanted)
        def _(both=both):
            for copy in both:
                copy.start()

    stacked_ref = price_ref.reshape(factors, dates, tiles, LANES)
    carried = carry_ref[...]
    for date in range(dates):
        level = jnp.exp(carried + own_refs[date][...])
        level_ref[date] = level
        stacked_ref[:, date] = level.reshape(factors, tiles, LANES)

    @pl.when(fits)
    def _():
        def group(step):
            first = (SETS // GROUP - 1 - step) * GROUP
            count = count_ref[first]

            def rows(r, nets):
                nets = [list(n) for n in nets]
                packs = index_ref.at[pl.ds(r * SETS + first, GROUP)]
                for u in range(2):
                    at = pl.ds(r * (2 * SETS) + u * SETS + first, GROUP)
                    strikes, weights = limit_ref.at[at], weight_ref.at[at]
                    for j in range(GROUP):
                        index = packs[j] >> SHIFT if u else packs[j] & ((1 << SHIFT) - 1)
                        strike, weight = strikes[j], weights[j]
                        for date in range(dates):
                            price = price_ref[pl.ds(pl.multiple_of(index + date * tiles, 8), tiles), :]
                            nets[date][j] += weight * jnp.maximum(price - strike, 0.0)
                return tuple(tuple(n) for n in nets)

            zero = jnp.zeros((tiles, LANES), jnp.float32)
            nets = lax.fori_loop(
                0, (count + 1) // 2, rows, ((zero,) * GROUP,) * dates
            )
            for date in range(dates):
                for part in range(GROUP // 8):
                    eight = [jnp.maximum(nets[date][part * 8 + i], 0.0) for i in range(8)]
                    at = pl.ds(pl.multiple_of(first + part * 8, 8), 8)
                    sum_ref[date, at, :] = over_sublanes(eight)
            return step + 1

        step = 0
        for part, (wanted, both) in enumerate(copies):

            @pl.when(wanted)
            def _(both=both):
                for copy in both:
                    copy.wait()

            def more(step, limit=2 * (PAIRS // PARTS) * (part + 1)):
                last = jnp.maximum(SETS // GROUP - 1 - step, 0)
                return (step < SETS // GROUP) & (count_ref[last * GROUP] <= limit)

            step = lax.while_loop(more, group, step)
        ones = jnp.ones((8, LANES), jnp.bfloat16)
        lines = []
        for date in range(dates):
            lines.append(sum(dot_last(ones, p.astype(jnp.bfloat16)) for p in pieces(sum_ref[date]))[:1])
        total = jnp.concatenate(lines + [jnp.zeros((16 - dates, SETS), jnp.float32)], axis=0)
        moved = moves(place_ref[...])
        parts = [jnp.dot(p.astype(jnp.bfloat16), moved, preferred_element_type=jnp.float32) for p in pieces(total)]
        out_ref[...] = (parts[0] + (parts[1] + parts[2]))[:dates]

    @pl.when(largest > ROWS)
    def _():
        pltpu.sync_copy(factor_hbm, factor_s)
        pltpu.sync_copy(set_hbm, set_s)
        pltpu.sync_copy(notional_hbm, notional_s)
        pltpu.sync_copy(strike_hbm, strike_s)

        def one_date(date, carry):
            net_ref[...] = jnp.zeros_like(net_ref)

            def trade(t, carry):
                price = level_ref[date, pl.ds(factor_s[t], 1), :]
                at = pl.ds(set_s[t], 1)
                net_ref[at, :] += notional_s[t] * jnp.maximum(price - strike_s[t], 0.0)
                return carry

            lax.fori_loop(0, factor_s.shape[0], trade, 0)
            sums = jnp.zeros((8, SETS), jnp.float32)
            ones = jnp.ones((8, LANES), jnp.bfloat16)
            for tile in range(tiles):
                for p in pieces(jnp.maximum(net_ref[:, tile * LANES : (tile + 1) * LANES], 0.0)):
                    sums += dot_last(ones, p.astype(jnp.bfloat16))
            out_ref[pl.ds(date, 1), :] = sums[:1]
            return carry

        lax.fori_loop(0, dates, one_date, 0)


def exposures(built, before, first, second, trades):
    index, level, weight, place, count = built
    dates, (factors, paths) = 2, first.shape
    vmem, hbm = pl.BlockSpec(memory_space=pltpu.VMEM), pl.BlockSpec(memory_space=pl.ANY)
    number = trades[0].shape
    return pl.pallas_call(
        exposure_kernel,
        out_shape=jax.ShapeDtypeStruct((dates, SETS), jnp.float32),
        in_specs=[pl.BlockSpec(memory_space=pltpu.SMEM)] + [hbm] * 3 + [vmem] * 4 + [hbm] * 4,
        out_specs=vmem,
        scratch_shapes=[
            pltpu.SMEM((PAIRS * SETS,), jnp.int32),
            pltpu.SMEM((PAIRS * 2 * SETS,), jnp.float32),
            pltpu.SMEM((PAIRS * 2 * SETS,), jnp.float32),
            pltpu.SemaphoreType.DMA((PARTS, 3)),
            pltpu.VMEM((dates, factors, paths), jnp.float32),
            pltpu.VMEM((factors * dates * (paths // LANES), LANES), jnp.float32),
            pltpu.VMEM((dates, SETS, LANES), jnp.float32),
            pltpu.VMEM((SETS, paths), jnp.float32),
            pltpu.SMEM(number, jnp.int32),
            pltpu.SMEM(number, jnp.int32),
            pltpu.SMEM(number, jnp.float32),
            pltpu.SMEM(number, jnp.float32),
        ],
        compiler_params=pltpu.CompilerParams(vmem_limit_bytes=12 << 20),
        name="exposures",
    )(count.reshape(SETS), index.reshape(-1), level.reshape(-1), weight.reshape(-1), place, before, first, second, *trades)


def pack_kernel(owner_ref, cholesky_ref, out_ref):
    dates, half = cholesky_ref.shape[0] // out_ref.shape[0], LANES // 2
    factors = out_ref.shape[0]
    section, holder = lax.axis_index("section"), lax.axis_index("paths")
    out_ref[...] = jnp.zeros_like(out_ref)
    for date in range(dates):
        block = cholesky_ref[pl.ds(date * factors, factors), 0, :]
        mine = owner_ref[section * dates + date] == holder
        out_ref[:, date * half : date * half + factors] = jnp.where(mine, block, 0.0)


def packed_blocks(cholesky, owner):
    dates, _, factors, _ = cholesky.shape
    return pl.pallas_call(
        pack_kernel,
        out_shape=jax.ShapeDtypeStruct((factors, LANES), jnp.float32),
        in_specs=[pl.BlockSpec(memory_space=pltpu.SMEM), pl.BlockSpec(memory_space=pltpu.VMEM)],
        out_specs=pl.BlockSpec(memory_space=pltpu.VMEM),
        compiler_params=pltpu.CompilerParams(vmem_limit_bytes=4 << 20),
        name="pack",
    )(owner, cholesky.transpose(0, 2, 1, 3).reshape(dates * factors, 1, factors))


def carried_in(total, fill):
    sections, section = lax.axis_size("section"), lax.axis_index("section")
    before = jnp.zeros_like(total)
    middle = total.shape[1] // 2
    odd = (section & 1) == 1
    distance, filled = 1, None
    while distance < sections:
        last = 2 * distance == sections
        pairs = [(i, i ^ distance) for i in range(sections) if not (last and i & distance)]
        if distance == 1:
            got = lax.ppermute(total, "section", pairs)
        else:
            half = jnp.where(odd, total[:, middle:], total[:, :middle])
            if filled is None:
                half, filled = fill(half)
            own = lax.ppermute(half, "section", pairs)
            own, filled = lax.optimization_barrier((own, filled))
            other = lax.ppermute(own, "section", [(i, i ^ 1) for i in range(sections)])
            got = jnp.concatenate([jnp.where(odd, other, own), jnp.where(odd, own, other)], axis=1)
        before = before + jnp.where((section & distance) != 0, got, 0.0)
        if not last:
            total = total + got
        distance *= 2
    return before, fill(total)[1] if filled is None else filled


def shards(normal_draws, cholesky, log_spot, owner, trade_factor, trade_set, notional, strike):
    dates, factors, paths = normal_draws.shape
    half = LANES // 2
    trades = (trade_factor, trade_set, notional, strike)
    blocks = summed(packed_blocks(cholesky, owner), "paths")
    draws = jnp.pad(normal_draws, ((0, 0), (0, half - factors), (0, 0))).reshape(dates * half, paths)
    first, second = (
        jnp.dot(
            blocks[:, : (date + 1) * half],
            draws[: (date + 1) * half],
            precision=lax.Precision.HIGHEST,
            preferred_element_type=jnp.float32,
        )
        for date in range(dates)
    )

    def fill(ready):
        spot = log_spot[:, None]
        ready, *own, tied = lax.optimization_barrier((ready, first + spot, second + spot, trades))
        return ready, (own, tables(dates * paths // LANES, *tied))

    before, (levels, built) = carried_in(second, fill)
    sums = exposures(built, before, *levels, trades)
    totals = summed(sums, "paths")
    return totals / (paths * lax.axis_size("paths"))


def solution(mesh):
    placed = (P("section", None, "paths"), P("section", "paths", None, None)) + (P(),) * 6
    return jax.shard_map(
        shards, mesh=mesh, in_specs=placed, out_specs=P("section", None), check_vma=False
    )
```

```python
import functools

import jax
import jax.numpy as jnp
from jax import lax
from jax.experimental import pallas as pl
from jax.experimental.pallas import tpu as pltpu
from jax.sharding import PartitionSpec as P

SETS = 512
LANES = 128
LOW = 128.0
BLOCKS = SETS // LANES
CHUNK = 2 * LANES
ROWS = 32
PAIRS = ROWS // 2
SHIFT = 16
GROUP = 16
PARTS = 8


def summed(part, axis):
    size = lax.axis_size(axis)
    if size & (size - 1):
        return lax.psum(part, axis)

    def swapped(distance):
        return lax.ppermute(part, axis, [(i, i ^ distance) for i in range(size)])

    distance = size // 2
    while distance > 2:
        part = part + swapped(distance)
        distance //= 2
    if size >= 4:
        return (part + swapped(1)) + (swapped(2) + swapped(3))
    return part + swapped(1) if size == 2 else part


def pieces(value):
    first = value.astype(jnp.bfloat16).astype(jnp.float32)
    rest = value - first
    second = rest.astype(jnp.bfloat16).astype(jnp.float32)
    return first, second, rest - second


def dot_last(a, b):
    return lax.dot_general(a, b, (((1,), (1,)), ((), ())), preferred_element_type=jnp.float32)


def iota(shape, dim):
    return lax.broadcasted_iota(jnp.int32, shape, dim)


def moves(place):
    hot = iota((SETS, SETS), 0).astype(jnp.float32) == place
    return hot.astype(jnp.float32).astype(jnp.bfloat16)


def table_kernel(
    step, factor_ref, set_ref, notional_ref, level_ref,
    index_ref, strike_ref, weight_ref, place_ref, count_ref,
    before_ref, base_ref, table_ref,
):
    chunks = factor_ref.shape[0] // 2
    before_ref[...] = (iota((CHUNK, CHUNK), 0) < iota((CHUNK, CHUNK), 1)).astype(jnp.bfloat16)
    base_ref[...] = jnp.zeros_like(base_ref)
    table_ref[...] = jnp.zeros_like(table_ref)
    set_ids = iota((SETS, LANES), 0)
    rows_at = iota((ROWS, LANES), 0)
    row_ids = jnp.where(rows_at < PAIRS, 2 * rows_at, 2 * (rows_at - PAIRS) + 1).astype(jnp.float32)

    def chunk(turn, carry):
        masks, rows = [], []
        for half in range(2):
            masks.append(set_ids == set_ref[pl.ds(2 * turn + half, 1), :])
        hot = jnp.concatenate([m.astype(jnp.float32).astype(jnp.bfloat16) for m in masks], axis=1)
        earlier = jnp.dot(hot, before_ref[...], preferred_element_type=jnp.float32)
        base = base_ref[...]
        for half in range(2):
            rank = jnp.sum(
                jnp.where(masks[half], earlier[:, half * LANES : (half + 1) * LANES] + base, 0.0),
                axis=0, keepdims=True,
            )
            here = row_ids == rank
            own = pl.ds(2 * turn + half, 1)
            values = (
                (factor_ref[own, :].astype(jnp.float32),)
                + pieces(level_ref[own, :])
                + pieces(notional_ref[own, :])
            )
            rows.append([jnp.where(here, v, 0.0) for v in values])
        parts = [
            jnp.concatenate([rows[0][i], rows[1][i]], axis=1).astype(jnp.bfloat16)
            for i in range(len(rows[0]))
        ]
        parts.append(jnp.ones((16, CHUNK), jnp.bfloat16))
        table_ref[...] += dot_last(jnp.concatenate(parts, axis=0), hot)
        last = earlier[:, CHUNK - 1 :] + masks[1][:, LANES - 1 :].astype(jnp.float32)
        base_ref[...] = base + jnp.broadcast_to(last, (SETS, LANES))
        return carry

    lax.fori_loop(0, chunks, chunk, 0, unroll=4)
    table = table_ref[...]
    counts = table[7 * ROWS : 7 * ROWS + 1, :]
    base = base_ref[...]
    places = []
    for block in range(BLOCKS):
        own = counts[:, block * LANES : (block + 1) * LANES]
        mine = iota((SETS, LANES), 1) + block * LANES
        ahead = (base > own) | ((base == own) & (set_ids < mine))
        places.append(jnp.sum(jnp.where(ahead, 1.0, 0.0), axis=0, keepdims=True))
    place = jnp.concatenate(places, axis=1)
    moved = moves(place)
    place_ref[...] = place
    table = dot_last(table[: 7 * ROWS, :].astype(jnp.bfloat16), moved)
    index = table[:ROWS, :].astype(jnp.int32)
    index = (index[:PAIRS] + (index[PAIRS:] << SHIFT)) * step
    strike = table[ROWS : 2 * ROWS] + (table[2 * ROWS : 3 * ROWS] + table[3 * ROWS : 4 * ROWS])
    weight = table[4 * ROWS : 5 * ROWS] + (table[5 * ROWS : 6 * ROWS] + table[6 * ROWS : 7 * ROWS])
    for block in range(BLOCKS):
        own = slice(block * LANES, (block + 1) * LANES)
        index_ref[:, block, :] = index[:, own]
        for half in range(2):
            at = slice(half * PAIRS, (half + 1) * PAIRS)
            strike_ref[:, half * BLOCKS + block, :] = strike[at, own]
            weight_ref[:, half * BLOCKS + block, :] = weight[at, own]
    exact = jnp.concatenate([(counts - LOW * jnp.floor(counts / LOW)), jnp.floor(counts / LOW)] + [jnp.zeros((14, SETS), jnp.float32)], axis=0)
    ordered = dot_last(exact.astype(jnp.bfloat16), moved)
    count_ref[...] = (ordered[:1] + LOW * ordered[1:2]).astype(jnp.int32)


def tables(step, trade_factor, trade_set, notional, strike):
    lines = trade_factor.shape[0] // LANES
    packed = [a.reshape(lines, LANES) for a in (trade_factor, trade_set, notional, strike)]
    vmem = pl.BlockSpec(memory_space=pltpu.VMEM)
    return pl.pallas_call(
        functools.partial(table_kernel, step),
        out_shape=(
            jax.ShapeDtypeStruct((PAIRS, BLOCKS, LANES), jnp.int32),
            jax.ShapeDtypeStruct((PAIRS, 2 * BLOCKS, LANES), jnp.float32),
            jax.ShapeDtypeStruct((PAIRS, 2 * BLOCKS, LANES), jnp.float32),
            jax.ShapeDtypeStruct((1, SETS), jnp.float32),
            jax.ShapeDtypeStruct((1, SETS), jnp.int32),
        ),
        in_specs=[vmem] * 4,
        out_specs=(vmem,) * 5,
        scratch_shapes=[
            pltpu.VMEM((CHUNK, CHUNK), jnp.bfloat16),
            pltpu.VMEM((SETS, LANES), jnp.float32),
            pltpu.VMEM((7 * ROWS + 16, SETS), jnp.float32),
        ],
        cost_estimate=pl.CostEstimate(
            flops=2 * trade_factor.shape[0] * SETS * 500, transcendentals=0, bytes_accessed=1 << 20
        ),
        compiler_params=pltpu.CompilerParams(vmem_limit_bytes=8 << 20),
        name="tables",
    )(*packed)


def over_sublanes(nets):
    row = iota((8, LANES), 0)
    for bit in (4, 2, 1):
        low = (row & bit) == 0
        nets = [
            jnp.where(low, a, pltpu.roll(b, bit, 0)) + jnp.where(low, pltpu.roll(a, 8 - bit, 0), b)
            for a, b in zip(nets[: len(nets) // 2], nets[len(nets) // 2 :])
        ]
    return nets[0]


def exposure_kernel(
    count_ref, index_hbm, level_hbm, weight_hbm, place_ref, carry_ref, first_ref, second_ref,
    factor_hbm, set_hbm, notional_hbm, strike_hbm,
    out_ref,
    index_ref, limit_ref, weight_ref, copied, level_ref, price_ref, sum_ref, net_ref, factor_s, set_s, notional_s, strike_s,
):
    own_refs = (first_ref, second_ref)
    dates, (factors, paths) = len(own_refs), first_ref.shape
    tiles = paths // LANES
    largest = count_ref[0]
    fits = largest <= ROWS
    copies = []
    for part in range(PARTS):
        each = PAIRS // PARTS
        wanted = fits & ((largest > 2 * each * part) | (part == 0))
        both = []
        for source, target, row in ((index_hbm, index_ref, SETS), (level_hbm, limit_ref, 2 * SETS), (weight_hbm, weight_ref, 2 * SETS)):
            at = pl.ds(part * each * row, each * row)
            both.append(pltpu.make_async_copy(source.at[at], target.at[at], copied.at[part, len(both)]))
        copies.append((wanted, both))

        @pl.when(wanted)
        def _(both=both):
            for copy in both:
                copy.start()

    stacked_ref = price_ref.reshape(factors, dates, tiles, LANES)
    carried = carry_ref[...]
    for date in range(dates):
        level = jnp.exp(carried + own_refs[date][...])
        level_ref[date] = level
        stacked_ref[:, date] = level.reshape(factors, tiles, LANES)

    @pl.when(fits)
    def _():
        def group(step):
            first = (SETS // GROUP - 1 - step) * GROUP
            count = count_ref[first]

            def rows(r, nets):
                nets = [list(n) for n in nets]
                packs = index_ref.at[pl.ds(r * SETS + first, GROUP)]
                for u in range(2):
                    at = pl.ds(r * (2 * SETS) + u * SETS + first, GROUP)
                    strikes, weights = limit_ref.at[at], weight_ref.at[at]
                    for j in range(GROUP):
                        index = packs[j] >> SHIFT if u else packs[j] & ((1 << SHIFT) - 1)
                        strike, weight = strikes[j], weights[j]
                        for date in range(dates):
                            price = price_ref[pl.ds(pl.multiple_of(index + date * tiles, 8), tiles), :]
                            nets[date][j] += weight * jnp.maximum(price - strike, 0.0)
                return tuple(tuple(n) for n in nets)

            zero = jnp.zeros((tiles, LANES), jnp.float32)
            nets = lax.fori_loop(
                0, (count + 1) // 2, rows, ((zero,) * GROUP,) * dates
            )
            for date in range(dates):
                for part in range(GROUP // 8):
                    eight = [jnp.maximum(nets[date][part * 8 + i], 0.0) for i in range(8)]
                    at = pl.ds(pl.multiple_of(first + part * 8, 8), 8)
                    sum_ref[date, at, :] = over_sublanes(eight)
            return step + 1

        step = 0
        for part, (wanted, both) in enumerate(copies):

            @pl.when(wanted)
            def _(both=both):
                for copy in both:
                    copy.wait()

            def more(step, limit=2 * (PAIRS // PARTS) * (part + 1)):
                last = jnp.maximum(SETS // GROUP - 1 - step, 0)
                return (step < SETS // GROUP) & (count_ref[last * GROUP] <= limit)

            step = lax.while_loop(more, group, step)
        ones = jnp.ones((8, LANES), jnp.bfloat16)
        lines = []
        for date in range(dates):
            lines.append(sum(dot_last(ones, p.astype(jnp.bfloat16)) for p in pieces(sum_ref[date]))[:1])
        total = jnp.concatenate(lines + [jnp.zeros((16 - dates, SETS), jnp.float32)], axis=0)
        moved = moves(place_ref[...])
        parts = [jnp.dot(p.astype(jnp.bfloat16), moved, preferred_element_type=jnp.float32) for p in pieces(total)]
        out_ref[...] = (parts[0] + (parts[1] + parts[2]))[:dates]

    @pl.when(largest > ROWS)
    def _():
        pltpu.sync_copy(factor_hbm, factor_s)
        pltpu.sync_copy(set_hbm, set_s)
        pltpu.sync_copy(notional_hbm, notional_s)
        pltpu.sync_copy(strike_hbm, strike_s)

        def one_date(date, carry):
            net_ref[...] = jnp.zeros_like(net_ref)

            def trade(t, carry):
                price = level_ref[date, pl.ds(factor_s[t], 1), :]
                at = pl.ds(set_s[t], 1)
                net_ref[at, :] += notional_s[t] * jnp.maximum(price - strike_s[t], 0.0)
                return carry

            lax.fori_loop(0, factor_s.shape[0], trade, 0)
            sums = jnp.zeros((8, SETS), jnp.float32)
            ones = jnp.ones((8, LANES), jnp.bfloat16)
            for tile in range(tiles):
                for p in pieces(jnp.maximum(net_ref[:, tile * LANES : (tile + 1) * LANES], 0.0)):
                    sums += dot_last(ones, p.astype(jnp.bfloat16))
            out_ref[pl.ds(date, 1), :] = sums[:1]
            return carry

        lax.fori_loop(0, dates, one_date, 0)


def exposures(built, before, first, second, trades):
    index, level, weight, place, count = built
    dates, (factors, paths) = 2, first.shape
    vmem, hbm = pl.BlockSpec(memory_space=pltpu.VMEM), pl.BlockSpec(memory_space=pl.ANY)
    number = trades[0].shape
    return pl.pallas_call(
        exposure_kernel,
        out_shape=jax.ShapeDtypeStruct((dates, SETS), jnp.float32),
        in_specs=[pl.BlockSpec(memory_space=pltpu.SMEM)] + [hbm] * 3 + [vmem] * 4 + [hbm] * 4,
        out_specs=vmem,
        scratch_shapes=[
            pltpu.SMEM((PAIRS * SETS,), jnp.int32),
            pltpu.SMEM((PAIRS * 2 * SETS,), jnp.float32),
            pltpu.SMEM((PAIRS * 2 * SETS,), jnp.float32),
            pltpu.SemaphoreType.DMA((PARTS, 3)),
            pltpu.VMEM((dates, factors, paths), jnp.float32),
            pltpu.VMEM((factors * dates * (paths // LANES), LANES), jnp.float32),
            pltpu.VMEM((dates, SETS, LANES), jnp.float32),
            pltpu.VMEM((SETS, paths), jnp.float32),
            pltpu.SMEM(number, jnp.int32),
            pltpu.SMEM(number, jnp.int32),
            pltpu.SMEM(number, jnp.float32),
            pltpu.SMEM(number, jnp.float32),
        ],
        compiler_params=pltpu.CompilerParams(vmem_limit_bytes=12 << 20),
        name="exposures",
    )(count.reshape(SETS), index.reshape(-1), level.reshape(-1), weight.reshape(-1), place, before, first, second, *trades)


def pack_kernel(owner_ref, cholesky_ref, out_ref):
    dates, half = cholesky_ref.shape[0] // out_ref.shape[0], LANES // 2
    factors = out_ref.shape[0]
    section, holder = lax.axis_index("section"), lax.axis_index("paths")
    out_ref[...] = jnp.zeros_like(out_ref)
    for date in range(dates):
        block = cholesky_ref[pl.ds(date * factors, factors), 0, :]
        mine = owner_ref[section * dates + date] == holder
        out_ref[:, date * half : date * half + factors] = jnp.where(mine, block, 0.0)


def packed_blocks(cholesky, owner):
    dates, _, factors, _ = cholesky.shape
    return pl.pallas_call(
        pack_kernel,
        out_shape=jax.ShapeDtypeStruct((factors, LANES), jnp.float32),
        in_specs=[pl.BlockSpec(memory_space=pltpu.SMEM), pl.BlockSpec(memory_space=pltpu.VMEM)],
        out_specs=pl.BlockSpec(memory_space=pltpu.VMEM),
        compiler_params=pltpu.CompilerParams(vmem_limit_bytes=4 << 20),
        name="pack",
    )(owner, cholesky.transpose(0, 2, 1, 3).reshape(dates * factors, 1, factors))


def carried_in(total, fill):
    sections, section = lax.axis_size("section"), lax.axis_index("section")
    before = jnp.zeros_like(total)
    middle = total.shape[1] // 2
    odd = (section & 1) == 1
    distance, filled = 1, None
    while distance < sections:
        last = 2 * distance == sections
        pairs = [(i, i ^ distance) for i in range(sections) if not (last and i & distance)]
        if distance == 1:
            got = lax.ppermute(total, "section", pairs)
        else:
            half = jnp.where(odd, total[:, middle:], total[:, :middle])
            if filled is None:
                half, filled = fill(half)
            own = lax.ppermute(half, "section", pairs)
            own, filled = lax.optimization_barrier((own, filled))
            other = lax.ppermute(own, "section", [(i, i ^ 1) for i in range(sections)])
            got = jnp.concatenate([jnp.where(odd, other, own), jnp.where(odd, own, other)], axis=1)
        before = before + jnp.where((section & distance) != 0, got, 0.0)
        if not last:
            total = total + got
        distance *= 2
    return before, fill(total)[1] if filled is None else filled


def shards(normal_draws, cholesky, log_spot, owner, trade_factor, trade_set, notional, strike):
    dates, factors, paths = normal_draws.shape
    half = LANES // 2
    trades = (trade_factor, trade_set, notional, strike)
    blocks = summed(packed_blocks(cholesky, owner), "paths")
    draws = jnp.pad(normal_draws, ((0, 0), (0, half - factors), (0, 0))).reshape(dates * half, paths)
    first, second = (
        jnp.dot(
            blocks[:, : (date + 1) * half],
            draws[: (date + 1) * half],
            precision=lax.Precision.HIGHEST,
            preferred_element_type=jnp.float32,
        )
        for date in range(dates)
    )

    def fill(ready):
        spot = log_spot[:, None]
        ready, *own, tied = lax.optimization_barrier((ready, first + spot, second + spot, trades))
        return ready, (own, tables(dates * paths // LANES, *tied))

    before, (levels, built) = carried_in(second, fill)
    sums = exposures(built, before, *levels, trades)
    totals = summed(sums, "paths")
    return totals / (paths * lax.axis_size("paths"))


def solution(mesh):
    placed = (P("section", None, "paths"), P("section", "paths", None, None)) + (P(),) * 6
    return jax.shard_map(
        shards, mesh=mesh, in_specs=placed, out_specs=P("section", None), check_vma=False
    )
```

```python
import functools

import jax
import jax.numpy as jnp
from jax import lax
from jax.experimental import pallas as pl
from jax.experimental.pallas import tpu as pltpu
from jax.sharding import PartitionSpec as P

SETS = 512
LANES = 128
LOW = 128.0
BLOCKS = SETS // LANES
CHUNK = 2 * LANES
ROWS = 32
PAIRS = ROWS // 2
SHIFT = 16
GROUP = 16
PARTS = 8


def summed(part, axis):
    size = lax.axis_size(axis)
    if size & (size - 1):
        return lax.psum(part, axis)

    def swapped(distance):
        return lax.ppermute(part, axis, [(i, i ^ distance) for i in range(size)])

    distance = size // 2
    while distance > 2:
        part = part + swapped(distance)
        distance //= 2
    if size >= 4:
        return (part + swapped(1)) + (swapped(2) + swapped(3))
    return part + swapped(1) if size == 2 else part


def pieces(value):
    first = value.astype(jnp.bfloat16).astype(jnp.float32)
    rest = value - first
    second = rest.astype(jnp.bfloat16).astype(jnp.float32)
    return first, second, rest - second


def dot_last(a, b):
    return lax.dot_general(a, b, (((1,), (1,)), ((), ())), preferred_element_type=jnp.float32)


def iota(shape, dim):
    return lax.broadcasted_iota(jnp.int32, shape, dim)


def moves(place):
    hot = iota((SETS, SETS), 0).astype(jnp.float32) == place
    return hot.astype(jnp.float32).astype(jnp.bfloat16)


def table_kernel(
    step, factor_ref, set_ref, notional_ref, level_ref,
    index_ref, strike_ref, weight_ref, place_ref, count_ref,
    before_ref, base_ref, table_ref,
):
    chunks = factor_ref.shape[0] // 2
    before_ref[...] = (iota((CHUNK, CHUNK), 0) < iota((CHUNK, CHUNK), 1)).astype(jnp.bfloat16)
    base_ref[...] = jnp.zeros_like(base_ref)
    table_ref[...] = jnp.zeros_like(table_ref)
    set_ids = iota((SETS, LANES), 0)
    rows_at = iota((ROWS, LANES), 0)
    row_ids = jnp.where(rows_at < PAIRS, 2 * rows_at, 2 * (rows_at - PAIRS) + 1).astype(jnp.float32)

    def chunk(turn, carry):
        masks, rows = [], []
        for half in range(2):
            masks.append(set_ids == set_ref[pl.ds(2 * turn + half, 1), :])
        hot = jnp.concatenate([m.astype(jnp.float32).astype(jnp.bfloat16) for m in masks], axis=1)
        earlier = jnp.dot(hot, before_ref[...], preferred_element_type=jnp.float32)
        base = base_ref[...]
        for half in range(2):
            rank = jnp.sum(
                jnp.where(masks[half], earlier[:, half * LANES : (half + 1) * LANES] + base, 0.0),
                axis=0, keepdims=True,
            )
            here = row_ids == rank
            own = pl.ds(2 * turn + half, 1)
            values = (
                (factor_ref[own, :].astype(jnp.float32),)
                + pieces(level_ref[own, :])
                + pieces(notional_ref[own, :])
            )
            rows.append([jnp.where(here, v, 0.0) for v in values])
        parts = [
            jnp.concatenate([rows[0][i], rows[1][i]], axis=1).astype(jnp.bfloat16)
            for i in range(len(rows[0]))
        ]
        parts.append(jnp.ones((16, CHUNK), jnp.bfloat16))
        table_ref[...] += dot_last(jnp.concatenate(parts, axis=0), hot)
        last = earlier[:, CHUNK - 1 :] + masks[1][:, LANES - 1 :].astype(jnp.float32)
        base_ref[...] = base + jnp.broadcast_to(last, (SETS, LANES))
        return carry

    lax.fori_loop(0, chunks, chunk, 0, unroll=4)
    table = table_ref[...]
    counts = table[7 * ROWS : 7 * ROWS + 1, :]
    base = base_ref[...]
    places = []
    for block in range(BLOCKS):
        own = counts[:, block * LANES : (block + 1) * LANES]
        mine = iota((SETS, LANES), 1) + block * LANES
        ahead = (base > own) | ((base == own) & (set_ids < mine))
        places.append(jnp.sum(jnp.where(ahead, 1.0, 0.0), axis=0, keepdims=True))
    place = jnp.concatenate(places, axis=1)
    moved = moves(place)
    place_ref[...] = moved
    table = dot_last(table[: 7 * ROWS, :].astype(jnp.bfloat16), moved)
    index = table[:ROWS, :].astype(jnp.int32)
    index = (index[:PAIRS] + (index[PAIRS:] << SHIFT)) * step
    strike = table[ROWS : 2 * ROWS] + (table[2 * ROWS : 3 * ROWS] + table[3 * ROWS : 4 * ROWS])
    weight = table[4 * ROWS : 5 * ROWS] + (table[5 * ROWS : 6 * ROWS] + table[6 * ROWS : 7 * ROWS])
    for block in range(BLOCKS):
        own = slice(block * LANES, (block + 1) * LANES)
        index_ref[:, block, :] = index[:, own]
        for half in range(2):
            at = slice(half * PAIRS, (half + 1) * PAIRS)
            strike_ref[:, half * BLOCKS + block, :] = strike[at, own]
            weight_ref[:, half * BLOCKS + block, :] = weight[at, own]
    exact = jnp.concatenate([(counts - LOW * jnp.floor(counts / LOW)), jnp.floor(counts / LOW)] + [jnp.zeros((14, SETS), jnp.float32)], axis=0)
    ordered = dot_last(exact.astype(jnp.bfloat16), moved)
    count_ref[...] = (ordered[:1] + LOW * ordered[1:2]).astype(jnp.int32)


def tables(step, trade_factor, trade_set, notional, strike):
    lines = trade_factor.shape[0] // LANES
    packed = [a.reshape(lines, LANES) for a in (trade_factor, trade_set, notional, strike)]
    vmem = pl.BlockSpec(memory_space=pltpu.VMEM)
    return pl.pallas_call(
        functools.partial(table_kernel, step),
        out_shape=(
            jax.ShapeDtypeStruct((PAIRS, BLOCKS, LANES), jnp.int32),
            jax.ShapeDtypeStruct((PAIRS, 2 * BLOCKS, LANES), jnp.float32),
            jax.ShapeDtypeStruct((PAIRS, 2 * BLOCKS, LANES), jnp.float32),
            jax.ShapeDtypeStruct((SETS, SETS), jnp.bfloat16),
            jax.ShapeDtypeStruct((1, SETS), jnp.int32),
        ),
        in_specs=[vmem] * 4,
        out_specs=(vmem,) * 5,
        scratch_shapes=[
            pltpu.VMEM((CHUNK, CHUNK), jnp.bfloat16),
            pltpu.VMEM((SETS, LANES), jnp.float32),
            pltpu.VMEM((7 * ROWS + 16, SETS), jnp.float32),
        ],
        cost_estimate=pl.CostEstimate(
            flops=2 * trade_factor.shape[0] * SETS * 500, transcendentals=0, bytes_accessed=1 << 20
        ),
        compiler_params=pltpu.CompilerParams(vmem_limit_bytes=8 << 20),
        name="tables",
    )(*packed)


def over_sublanes(nets):
    row = iota((8, LANES), 0)
    for bit in (4, 2, 1):
        low = (row & bit) == 0
        nets = [
            jnp.where(low, a, pltpu.roll(b, bit, 0)) + jnp.where(low, pltpu.roll(a, 8 - bit, 0), b)
            for a, b in zip(nets[: len(nets) // 2], nets[len(nets) // 2 :])
        ]
    return nets[0]


def exposure_kernel(
    count_hbm, index_hbm, level_hbm, weight_hbm, place_ref, carry_ref, first_ref, second_ref,
    factor_hbm, set_hbm, notional_hbm, strike_hbm,
    out_ref,
    count_ref, index_ref, limit_ref, weight_ref, counted, copied, level_ref, price_ref, sum_ref, net_ref, factor_s, set_s, notional_s, strike_s,
):
    own_refs = (first_ref, second_ref)
    dates, (factors, paths) = len(own_refs), first_ref.shape
    tiles = paths // LANES
    counting = pltpu.make_async_copy(count_hbm, count_ref, counted)
    counting.start()
    copies = []
    for part in range(PARTS):
        each = PAIRS // PARTS
        both = []
        for source, target, row in (
            (index_hbm, index_ref, SETS), (level_hbm, limit_ref, 2 * SETS), (weight_hbm, weight_ref, 2 * SETS)
        ):
            at = pl.ds(part * each * row, each * row)
            both.append(pltpu.make_async_copy(source.at[at], target.at[at], copied.at[part, len(both)]))
        copies.append(both)
    for copy in copies[0]:
        copy.start()
    stacked_ref = price_ref.reshape(factors, dates, tiles, LANES)
    carried = carry_ref[...]
    for date in range(dates):
        level = jnp.exp(carried + own_refs[date][...])
        level_ref[date] = level
        stacked_ref[:, date] = level.reshape(factors, tiles, LANES)
    counting.wait()
    largest = count_ref[0]
    fits = largest <= ROWS
    wanted = [fits & (largest > 2 * (PAIRS // PARTS) * part) for part in range(PARTS)]
    for part in range(1, PARTS):

        @pl.when(wanted[part])
        def _(both=copies[part]):
            for copy in both:
                copy.start()

    for copy in copies[0]:
        copy.wait()

    @pl.when(fits)
    def _():
        def group(step):
            first = (SETS // GROUP - 1 - step) * GROUP
            count = count_ref[first]

            def rows(r, nets):
                nets = [list(n) for n in nets]
                packs = index_ref.at[pl.ds(r * SETS + first, GROUP)]
                for u in range(2):
                    at = pl.ds(r * (2 * SETS) + u * SETS + first, GROUP)
                    strikes, weights = limit_ref.at[at], weight_ref.at[at]
                    for j in range(GROUP):
                        index = packs[j] >> SHIFT if u else packs[j] & ((1 << SHIFT) - 1)
                        strike, weight = strikes[j], weights[j]
                        for date in range(dates):
                            price = price_ref[pl.ds(pl.multiple_of(index + date * tiles, 8), tiles), :]
                            nets[date][j] += weight * jnp.maximum(price - strike, 0.0)
                return tuple(tuple(n) for n in nets)

            zero = jnp.zeros((tiles, LANES), jnp.float32)
            nets = lax.fori_loop(
                0, (count + 1) // 2, rows, ((zero,) * GROUP,) * dates
            )
            for date in range(dates):
                for part in range(GROUP // 8):
                    eight = [jnp.maximum(nets[date][part * 8 + i], 0.0) for i in range(8)]
                    at = pl.ds(pl.multiple_of(first + part * 8, 8), 8)
                    sum_ref[date, at, :] = over_sublanes(eight)
            return step + 1

        step = 0
        for part, both in enumerate(copies):
            if part:

                @pl.when(wanted[part])
                def _(both=both):
                    for copy in both:
                        copy.wait()

            def more(step, limit=2 * (PAIRS // PARTS) * (part + 1)):
                last = jnp.maximum(SETS // GROUP - 1 - step, 0)
                return (step < SETS // GROUP) & (count_ref[last * GROUP] <= limit)

            step = lax.while_loop(more, group, step)
        ones = jnp.ones((8, LANES), jnp.bfloat16)
        lines = []
        for date in range(dates):
            lines.append(sum(dot_last(ones, p.astype(jnp.bfloat16)) for p in pieces(sum_ref[date]))[:1])
        total = jnp.concatenate(lines + [jnp.zeros((16 - dates, SETS), jnp.float32)], axis=0)
        moved = place_ref[...]
        parts = [jnp.dot(p.astype(jnp.bfloat16), moved, preferred_element_type=jnp.float32) for p in pieces(total)]
        out_ref[...] = (parts[0] + (parts[1] + parts[2]))[:dates]

    @pl.when(largest > ROWS)
    def _():
        pltpu.sync_copy(factor_hbm, factor_s)
        pltpu.sync_copy(set_hbm, set_s)
        pltpu.sync_copy(notional_hbm, notional_s)
        pltpu.sync_copy(strike_hbm, strike_s)

        def one_date(date, carry):
            net_ref[...] = jnp.zeros_like(net_ref)

            def trade(t, carry):
                price = level_ref[date, pl.ds(factor_s[t], 1), :]
                at = pl.ds(set_s[t], 1)
                net_ref[at, :] += notional_s[t] * jnp.maximum(price - strike_s[t], 0.0)
                return carry

            lax.fori_loop(0, factor_s.shape[0], trade, 0)
            sums = jnp.zeros((8, SETS), jnp.float32)
            ones = jnp.ones((8, LANES), jnp.bfloat16)
            for tile in range(tiles):
                for p in pieces(jnp.maximum(net_ref[:, tile * LANES : (tile + 1) * LANES], 0.0)):
                    sums += dot_last(ones, p.astype(jnp.bfloat16))
            out_ref[pl.ds(date, 1), :] = sums[:1]
            return carry

        lax.fori_loop(0, dates, one_date, 0)


def exposures(built, before, first, second, trades):
    index, level, weight, place, count = built
    dates, (factors, paths) = 2, first.shape
    vmem, hbm = pl.BlockSpec(memory_space=pltpu.VMEM), pl.BlockSpec(memory_space=pl.ANY)
    number = trades[0].shape
    return pl.pallas_call(
        exposure_kernel,
        out_shape=jax.ShapeDtypeStruct((dates, SETS), jnp.float32),
        in_specs=[hbm] * 4 + [vmem] * 4 + [hbm] * 4,
        out_specs=vmem,
        scratch_shapes=[
            pltpu.SMEM((SETS,), jnp.int32),
            pltpu.SMEM((PAIRS * SETS,), jnp.int32),
            pltpu.SMEM((PAIRS * 2 * SETS,), jnp.float32),
            pltpu.SMEM((PAIRS * 2 * SETS,), jnp.float32),
            pltpu.SemaphoreType.DMA,
            pltpu.SemaphoreType.DMA((PARTS, 3)),
            pltpu.VMEM((dates, factors, paths), jnp.float32),
            pltpu.VMEM((factors * dates * (paths // LANES), LANES), jnp.float32),
            pltpu.VMEM((dates, SETS, LANES), jnp.float32),
            pltpu.VMEM((SETS, paths), jnp.float32),
            pltpu.SMEM(number, jnp.int32),
            pltpu.SMEM(number, jnp.int32),
            pltpu.SMEM(number, jnp.float32),
            pltpu.SMEM(number, jnp.float32),
        ],
        compiler_params=pltpu.CompilerParams(vmem_limit_bytes=12 << 20),
        name="exposures",
    )(count.reshape(SETS), index.reshape(-1), level.reshape(-1), weight.reshape(-1), place, before, first, second, *trades)


def pack_kernel(owner_ref, cholesky_ref, out_ref):
    dates, half = cholesky_ref.shape[0] // out_ref.shape[0], LANES // 2
    factors = out_ref.shape[0]
    section, holder = lax.axis_index("section"), lax.axis_index("paths")
    out_ref[...] = jnp.zeros_like(out_ref)
    for date in range(dates):
        block = cholesky_ref[pl.ds(date * factors, factors), 0, :]
        mine = owner_ref[section * dates + date] == holder
        out_ref[:, date * half : date * half + factors] = jnp.where(mine, block, 0.0)


def packed_blocks(cholesky, owner):
    dates, _, factors, _ = cholesky.shape
    return pl.pallas_call(
        pack_kernel,
        out_shape=jax.ShapeDtypeStruct((factors, LANES), jnp.float32),
        in_specs=[pl.BlockSpec(memory_space=pltpu.SMEM), pl.BlockSpec(memory_space=pltpu.VMEM)],
        out_specs=pl.BlockSpec(memory_space=pltpu.VMEM),
        compiler_params=pltpu.CompilerParams(vmem_limit_bytes=4 << 20),
        name="pack",
    )(owner, cholesky.transpose(0, 2, 1, 3).reshape(dates * factors, 1, factors))


def carried_in(total, fill):
    sections, section = lax.axis_size("section"), lax.axis_index("section")
    before = jnp.zeros_like(total)
    middle = total.shape[1] // 2
    odd = (section & 1) == 1
    distance, filled = 1, None
    while distance < sections:
        last = 2 * distance == sections
        pairs = [(i, i ^ distance) for i in range(sections) if not (last and i & distance)]
        if distance == 1:
            got = lax.ppermute(total, "section", pairs)
        else:
            half = jnp.where(odd, total[:, middle:], total[:, :middle])
            if filled is None:
                half, filled = fill(half)
            own = lax.ppermute(half, "section", pairs)
            own, filled = lax.optimization_barrier((own, filled))
            other = lax.ppermute(own, "section", [(i, i ^ 1) for i in range(sections)])
            got = jnp.concatenate([jnp.where(odd, other, own), jnp.where(odd, own, other)], axis=1)
        before = before + jnp.where((section & distance) != 0, got, 0.0)
        if not last:
            total = total + got
        distance *= 2
    return before, fill(total)[1] if filled is None else filled


def shards(normal_draws, cholesky, log_spot, owner, trade_factor, trade_set, notional, strike):
    dates, factors, paths = normal_draws.shape
    half = LANES // 2
    trades = (trade_factor, trade_set, notional, strike)
    blocks = summed(packed_blocks(cholesky, owner), "paths")
    draws = jnp.pad(normal_draws, ((0, 0), (0, half - factors), (0, 0))).reshape(dates * half, paths)
    first, second = (
        jnp.dot(
            blocks[:, : (date + 1) * half],
            draws[: (date + 1) * half],
            precision=lax.Precision.HIGHEST,
            preferred_element_type=jnp.float32,
        )
        for date in range(dates)
    )

    def fill(ready):
        spot = log_spot[:, None]
        ready, *own, tied = lax.optimization_barrier((ready, first + spot, second + spot, trades))
        return ready, (own, tables(dates * paths // LANES, *tied))

    before, (levels, built) = carried_in(second, fill)
    sums = exposures(built, before, *levels, trades)
    totals = summed(sums, "paths")
    return totals / (paths * lax.axis_size("paths"))


def solution(mesh):
    placed = (P("section", None, "paths"), P("section", "paths", None, None)) + (P(),) * 6
    return jax.shard_map(
        shards, mesh=mesh, in_specs=placed, out_specs=P("section", None), check_vma=False
    )
```
